32 devices in a mesh: band: 8 (over z, y), grid: 4 (over x, core).
Axes of the slice: x: 2, y: 2, z: 4, core: 2. Of those that a mesh axis runs over, the one named last changes fastest.
Arguments:
- bands: bfloat16 [2, 16, 128, 128, 128], P(None, 'band', 'grid'), may hold values from -6 to 6
- occupations: float32 [16], P('band'), may hold values from 0.25 to 1
- external: float32 [128, 128, 128], P('grid'), may hold values from 0 to 2
- density_in: float32 [128, 128, 128], P('grid'), may hold values from -0.2 to 1.4
- prev_density: float32 [128, 128, 128], P('grid'), may hold values from 0 to 1.2
- prev_residual: float32 [128, 128, 128], P('grid'), may hold values from -1.3 to 0.3
- hist_density: float32 [5, 128, 128, 128], P(None, 'grid'), may hold values from 0 to 1
- hist_residual: float32 [5, 128, 128, 128], P(None, 'grid'), may hold values from -0.6 to 1
Outputs:
- density: float32 [128, 128, 128], P('grid')
- residual: float32 [128, 128, 128], P('grid')
The draws below stay inside these ranges and needn't reach their ends.
All inputs are finite; a program needn't handle non-finite values.
Results may differ from the reference program's by a relative error of at most 0.018.
The reference program's roundings to bfloat16 on the way count: a program that leaves them out, or rounds other values in their place, can miss the bound.
Values may be sent and summed in bfloat16 or wider, within the bound.
No kernel may reach another device: no remote copies, remote signals or barrier semaphores. Data moves between devices by JAX's collectives and lax.ppermute only.
A program may use at most 192 MiB of HBM per device.

```python
import math
import jax
import jax.numpy as jnp
from jax import lax

NG = 128
DEPTH = 6
ITERS = 3
BANDS = 16


def draw_density_in(key, part):
    jitter = jax.random.uniform(key, (NG, NG, NG), jnp.float32, -0.4, 0.4)
    position = jnp.arange(NG, dtype=jnp.float32)[:, None, None] / (NG - 1)
    return 0.2 + 0.8 * position + jitter


def draw_prev_residual(key, part):
    jitter = jax.random.uniform(jax.random.fold_in(key, 11), (NG, NG, NG), jnp.float32, -0.3, 0.3)
    position = jnp.arange(NG, dtype=jnp.float32)[:, None, None] / (NG - 1)
    return -(0.2 + 0.8 * position) + jitter


def draw_hist_residual(key, part):
    jitter = jax.random.uniform(jax.random.fold_in(key, 23), (DEPTH - 1, NG, NG, NG), jnp.float32, -0.3, 0.3)
    position = jnp.arange(NG, dtype=jnp.float32) / (NG - 1)
    order = DEPTH - 1 - jnp.arange(DEPTH - 1, dtype=jnp.float32)
    profile = 0.2 + 0.5 * jnp.cos(math.pi * order[:, None] * position[None, :])
    return profile[:, :, None, None] + jitter


def level_of(rng, shape, cuts, least, largest):
    level = 1.0
    for axis_at, parts in cuts:
        draws = jax.random.uniform(jax.random.fold_in(jax.random.fold_in(rng, 6), axis_at), (parts,), jnp.float32, least / len(cuts), largest / len(cuts))
        level = level * jnp.repeat(jnp.exp(draws), shape[axis_at] // parts).reshape((-1,) + (1,) * (len(shape) - 1 - axis_at))
    return level


def scatter_about(key, shape, spread, reach, shards=(), held_as=jnp.bfloat16):
    entries = jax.random.normal(key, shape, jnp.float32) * spread
    if len(shards) > 0:
        entries = level_of(key, shape, shards, -0.22, 0.18) * entries
    return jnp.clip(entries, min=-reach, max=reach).astype(held_as)


def setup_inputs(seed: int = 0) -> dict:
    streams_of = jax.random.split(jax.random.key(seed), 9)
    bands = scatter_about(streams_of[0], (2, BANDS, NG, NG, NG), 1.0, 6.0, ((1, 8), (2, 4)))
    occupations = jnp.clip(jnp.exp(math.log(1.0) - 1.3862944 * jax.random.uniform(streams_of[1], (BANDS,), jnp.float32) ** level_of(streams_of[1], (BANDS,), ((0, 8),), -0.2, 0.2)), 0.25, 1.0)
    external = jnp.clip(2.0 * jax.random.uniform(streams_of[2], (NG, NG, NG), jnp.float32) ** level_of(streams_of[2], (NG, NG, NG), ((0, 4),), -0.2, 0.2), 0.0, 2.0)
    density_in = draw_density_in(jax.random.fold_in(streams_of[8], 71), 0)
    prev_density = jnp.clip(1.2 * jax.random.uniform(streams_of[4], (NG, NG, NG), jnp.float32) ** level_of(streams_of[4], (NG, NG, NG), ((0, 4),), -0.2, 0.2), 0.0, 1.2)
    prev_residual = draw_prev_residual(jax.random.fold_in(streams_of[8], 71), 0)
    hist_density = jnp.clip(1.0 * jax.random.uniform(streams_of[6], (DEPTH - 1, NG, NG, NG), jnp.float32) ** level_of(streams_of[6], (DEPTH - 1, NG, NG, NG), ((1, 4),), -0.2, 0.2), 0.0, 1.0)
    hist_residual = draw_hist_residual(jax.random.fold_in(streams_of[8], 71), 0)
    return dict(bands=bands, occupations=occupations, external=external, density_in=density_in, prev_density=prev_density, prev_residual=prev_residual, hist_density=hist_density, hist_residual=hist_residual)


time_step = 0.25
energy_shift = 2.5
coupling = 1.0
mixing_weight = 0.5
ridge_share = 0.1
ridge_floor = 0.01
density_scale = 8.0
highest = lax.Precision.HIGHEST

def fourier_tables(length, frequency):
    positions = jnp.arange(length, dtype=jnp.int32)
    phase_index = positions[:, None] * frequency[None, :] % length
    angles = phase_index.astype(jnp.float32) * (2.0 * math.pi / length)
    unit_scale = 1.0 / math.sqrt(length)
    return ((jnp.cos(angles) * unit_scale).astype(jnp.bfloat16), (jnp.sin(angles) * unit_scale).astype(jnp.bfloat16))

def solve_definite(matrix, vector):
    extent = matrix.shape[0]
    factor_low = jnp.zeros_like(matrix)
    for column in range(extent):
        pivot_value = jnp.sqrt(matrix[column, column] - jnp.sum(factor_low[column, :column] * factor_low[column, :column]))
        factor_low = factor_low.at[column, column].set(pivot_value)
        for row_index in range(column + 1, extent):
            element = (matrix[row_index, column] - jnp.sum(factor_low[row_index, :column] * factor_low[column, :column])) / pivot_value
            factor_low = factor_low.at[row_index, column].set(element)
    middle = jnp.zeros_like(vector)
    for row_index in range(extent):
        element = (vector[row_index] - jnp.sum(factor_low[row_index, :row_index] * middle[:row_index])) / factor_low[row_index, row_index]
        middle = middle.at[row_index].set(element)
    result = jnp.zeros_like(vector)
    for row_index in reversed(range(extent)):
        element = (middle[row_index] - jnp.sum(factor_low[row_index + 1:, row_index] * result[row_index + 1:])) / factor_low[row_index, row_index]
        result = result.at[row_index].set(element)
    return result

def contract(operand, matrix):
    return jnp.einsum('abl,lk->abk', operand, matrix, precision=highest)

def along_axis(real_part, imag_part, cosine_part, sine_part, orientation, axis_index):
    cosine_wide = cosine_part.astype(jnp.float32)
    sine_wide = sine_part.astype(jnp.float32) * orientation
    real_moved = jnp.moveaxis(real_part.astype(jnp.float32), axis_index, -1)
    imag_moved = jnp.moveaxis(imag_part.astype(jnp.float32), axis_index, -1)
    out_real = contract(real_moved, cosine_wide) - contract(imag_moved, sine_wide)
    out_imag = contract(real_moved, sine_wide) + contract(imag_moved, cosine_wide)
    return (jnp.moveaxis(out_real, -1, axis_index), jnp.moveaxis(out_imag, -1, axis_index))

def band_step(real_part, imag_part, factor, kinetic, tables):
    cosine_part, sine_part = tables
    real_part = (real_part.astype(jnp.float32) * factor).astype(jnp.bfloat16)
    imag_part = (imag_part.astype(jnp.float32) * factor).astype(jnp.bfloat16)
    for axis_index in (2, 1):
        real_part, imag_part = along_axis(real_part, imag_part, cosine_part, sine_part, -1.0, axis_index)
        real_part = real_part.astype(jnp.bfloat16)
        imag_part = imag_part.astype(jnp.bfloat16)
    real_part, imag_part = along_axis(real_part, imag_part, cosine_part, sine_part, -1.0, 0)
    real_part = (real_part * kinetic).astype(jnp.bfloat16)
    imag_part = (imag_part * kinetic).astype(jnp.bfloat16)
    for axis_index in (0, 1, 2):
        real_part, imag_part = along_axis(real_part, imag_part, cosine_part.T, sine_part.T, 1.0, axis_index)
        real_part = real_part.astype(jnp.bfloat16)
        imag_part = imag_part.astype(jnp.bfloat16)
    return (real_part, imag_part)

def reference(bands, occupations, external, density_in, prev_density, prev_residual, hist_density, hist_residual):
    frequency = jnp.arange(-(NG // 4), NG // 4, dtype=jnp.int32)
    tables = fourier_tables(NG, frequency)
    squared = frequency.astype(jnp.float32) * frequency.astype(jnp.float32)
    quarter = NG / 4.0
    radius = squared[:, None, None] + squared[None, :, None] + squared[None, None, :]
    kinetic = jnp.exp(-time_step * radius / (quarter * quarter))
    cells_total = NG * NG * NG
    real_bands = bands[0]
    imag_bands = bands[1]
    density_now = density_in
    density_prev = prev_density
    residual_prev = prev_residual
    density_diffs = hist_density
    residual_diffs = hist_residual
    residual = density_in
    for iteration in range(ITERS):
        factor = jnp.exp(-time_step * (external + coupling * density_now - energy_shift))

        def one_band(accumulated, slices):
            real_part, imag_part, weight = slices
            real_part, imag_part = band_step(real_part, imag_part, factor, kinetic, tables)
            wide_real = real_part.astype(jnp.float32)
            wide_imag = imag_part.astype(jnp.float32)
            return (accumulated + weight * (wide_real * wide_real + wide_imag * wide_imag), (real_part, imag_part))
        accumulated, (real_bands, imag_bands) = lax.scan(one_band, jnp.zeros((NG, NG, NG), jnp.float32), (real_bands, imag_bands, occupations))
        density_out = accumulated * (density_scale / BANDS)
        residual = density_out - density_now
        density_diffs = jnp.concatenate([density_diffs[density_diffs.shape[0] - (DEPTH - 1):], (density_now - density_prev)[None]], axis=0)
        residual_diffs = jnp.concatenate([residual_diffs[residual_diffs.shape[0] - (DEPTH - 1):], (residual - residual_prev)[None]], axis=0)
        flat_diffs = residual_diffs.reshape(DEPTH, -1)
        gram_matrix = jnp.dot(flat_diffs, flat_diffs.T, precision=highest) / cells_total
        right_side = jnp.dot(flat_diffs, residual.reshape(-1), precision=highest) / cells_total
        ridge_value = ridge_share * jnp.trace(gram_matrix) / DEPTH + ridge_floor
        coeffs = solve_definite(gram_matrix + ridge_value * jnp.eye(DEPTH, dtype=jnp.float32), right_side)
        combined = density_diffs + mixing_weight * residual_diffs
        density_next = density_now + mixing_weight * residual - jnp.einsum('j,jxyz->xyz', coeffs, combined, precision=highest)
        density_prev = density_now
        residual_prev = residual
        density_now = density_next
    return (density_now, residual)
```

```python
import functools
import math

import jax
import jax.numpy as jnp
from jax import lax
from jax.experimental import pallas as pl
from jax.experimental.pallas import tpu as pltpu
from jax.sharding import PartitionSpec as P

DEPTH = 6
ITERS = 3
LANES = 128

time_step = 0.25
energy_shift = 2.5
mixing_weight = 0.5
ridge_share = 0.1
ridge_floor = 0.01
density_scale = 8.0


f32 = jnp.float32
bf16 = jnp.bfloat16


def fourier_tables(length, frequency):
    positions = jnp.arange(length, dtype=jnp.int32)
    phase_index = positions[:, None] * frequency[None, :] % length
    angles = phase_index.astype(f32) * (2.0 * math.pi / length)
    unit_scale = 1.0 / math.sqrt(length)
    return (
        (jnp.cos(angles) * unit_scale).astype(bf16),
        (jnp.sin(angles) * unit_scale).astype(bf16),
    )


def dot(a, b):
    return jnp.dot(a, b, preferred_element_type=f32)


def swap_halves(v):
    return pltpu.roll(v, v.shape[-1] // 2, v.ndim - 1)


def half_sign(shape, first):
    lane = lax.broadcasted_iota(jnp.int32, shape, len(shape) - 1)
    return jnp.where(lane < shape[-1] // 2, first, -first).astype(f32)


def units(refs, step, step_rows, row, count, me):
    half = refs[0].shape[1]
    assert step_rows % (2 * half) == 0
    unit = min(count, half)
    for at in range(0, count, unit):
        block, within = divmod(row + at, 2 * half)
        which, offset = divmod(within, half)
        block = lax.bitwise_xor(step * (step_rows // (2 * half)) + block, me)
        yield refs[which].at[block, pl.ds(offset, unit), :], at, unit


def read_rows(*where):
    out = [ref[...] for ref, _, _ in units(*where)]
    return out[0] if len(out) == 1 else jnp.concatenate(out, axis=0)


def write_rows(refs, step, step_rows, row, value, me):
    for ref, at, unit in units(refs, step, step_rows, row, value.shape[0], me):
        ref[...] = value[at : at + unit]


def solve_rows(gram, rhs):
    n = len(rhs)
    trace = gram[0][0]
    for j in range(1, n):
        trace = trace + gram[j][j]
    ridge = ridge_share * trace / n + ridge_floor
    a = [[gram[j][k] + ridge if j == k else gram[j][k] for k in range(n)] for j in range(n)]
    low = [[None] * n for _ in range(n)]
    diag = [None] * n
    inv = [None] * n
    for j in range(n):
        value = a[j][j]
        scaled = []
        for k in range(j):
            s = low[j][k] * diag[k]
            scaled.append(s)
            value = value - low[j][k] * s
        diag[j] = value
        inv[j] = 1.0 / value
        for r in range(j + 1, n):
            e = a[r][j]
            for k in range(j):
                e = e - low[r][k] * scaled[k]
            low[r][j] = e * inv[j]
    mid = []
    for j in range(n):
        e = rhs[j]
        for k in range(j):
            e = e - low[j][k] * mid[k]
        mid.append(e)
    out = [None] * n
    for j in reversed(range(n)):
        e = mid[j] * inv[j]
        for k in range(j + 1, n):
            e = e - low[k][j] * out[k]
        out[j] = e
    return out


def pair_index(n):
    return {(j, k): i for i, (j, k) in enumerate((j, k) for j in range(n) for k in range(j, n))}


def finish_stats(stats_ref, carry_ref, first, cells):
    total = stats_ref[0]
    for d in range(1, stats_ref.shape[0]):
        total = total + stats_ref[d]
    total = jnp.broadcast_to(jnp.sum(total, axis=1, keepdims=True), total.shape) * (1.0 / cells)
    n = DEPTH
    gram = [[None] * n for _ in range(n)]
    kept = pair_index(n - 1)
    for (j, k), i in kept.items():
        value = total[2 * n + i : 2 * n + i + 1] if first else carry_ref[i : i + 1, :]
        gram[j][k] = value
        gram[k][j] = value
    for j in range(n):
        value = total[j : j + 1]
        gram[j][n - 1] = value
        gram[n - 1][j] = value
    rhs = [total[n + j : n + j + 1] for j in range(n)]
    return gram, rhs


def stat_rows(first):
    rows = 2 * DEPTH + (DEPTH * (DEPTH - 1) // 2 if first else 0)
    return -(-rows // 8) * 8


CARRY_ROWS = 16


def combine_kernel(r_ref, q_ref, s_ref):
    s_ref[...] = (r_ref[...] + mixing_weight * q_ref[...]).astype(s_ref.dtype)


def combine(hist_density, hist_residual, parts):
    depth, rows, lanes = hist_density.shape
    block = rows // parts
    spec = pl.BlockSpec((depth, block, lanes), lambda s: (0, s, 0))
    return pl.pallas_call(
        combine_kernel,
        grid=(parts,),
        in_specs=[spec, spec],
        out_specs=spec,
        out_shape=jax.ShapeDtypeStruct((depth, rows, lanes), bf16),
        compiler_params=pltpu.CompilerParams(vmem_limit_bytes=24 << 20),
        cost_estimate=pl.CostEstimate(
            flops=rows * lanes * depth * 200, bytes_accessed=rows * lanes * depth * 10, transcendentals=0
        ),
        name="combine",
    )(hist_density, hist_residual)


def row_sum(v):
    return jnp.sum(v, axis=0, keepdims=True)


def dots_kernel(first, me_ref, *refs):
    q_count = DEPTH - 1
    rho_ref, in_ref, prev_ref = refs[:3]
    refs = refs[3:]
    if first:
        hist_ref = refs[0]
        refs = refs[1:]
        q = [hist_ref[j] for j in range(q_count)]
    else:
        q = [refs[j][...] for j in range(q_count)]
        refs = refs[q_count:]
    stats_ref, newest_ref, res_ref = refs
    res = rho_ref[...].astype(f32) - in_ref[...]
    newest = res - prev_ref[...]
    newest_ref[...] = newest
    res_ref[...] = res
    rows = [row_sum(v * newest) for v in q] + [row_sum(newest * newest)]
    rows += [row_sum(v * res) for v in q] + [row_sum(newest * res)]
    if first:
        for j, k in pair_index(q_count):
            rows.append(row_sum(q[j] * q[k]))
    stats_ref[...] = jnp.zeros_like(stats_ref)
    for i, v in enumerate(rows):
        stats_ref[i : i + 1, :] = v


def dots(first, me, rho_shard, rho_in, prev_res, residuals):
    block = rho_shard.shape[0]
    mine = pl.BlockSpec((block, LANES), lambda s, m: (m[0], 0))
    whole = pl.BlockSpec((block, LANES), lambda s, m: (0, 0))
    if first:
        hist = [residuals]
        hist_specs = [pl.BlockSpec((DEPTH - 1, block, LANES), lambda s, m: (0, m[0], 0))]
    else:
        hist = list(residuals)
        hist_specs = [
            pl.BlockSpec((None, block, LANES), functools.partial(lambda j, s, m: (j, m[0], 0), r[1]))
            if isinstance(r, tuple)
            else whole
            for r in hist
        ]
        hist = [r[0] if isinstance(r, tuple) else r for r in hist]
    rows = stat_rows(first)
    return pl.pallas_call(
        functools.partial(dots_kernel, first),
        grid_spec=pltpu.PrefetchScalarGridSpec(
            num_scalar_prefetch=1,
            grid=(1,),
            in_specs=[whole, mine, mine if first else whole] + hist_specs,
            out_specs=[
                pl.BlockSpec((rows, LANES), lambda s, m: (0, 0)),
                whole,
                whole,
            ],
        ),
        out_shape=[
            jax.ShapeDtypeStruct((rows, LANES), f32),
            jax.ShapeDtypeStruct((block, LANES), f32),
            jax.ShapeDtypeStruct((block, LANES), f32),
        ],
        compiler_params=pltpu.CompilerParams(vmem_limit_bytes=16 << 20),
        cost_estimate=pl.CostEstimate(flops=10**7, bytes_accessed=block * LANES * 32, transcendentals=0),
        name="dots",
    )(me, rho_shard, rho_in, prev_res, *hist)


def mix_plane(me, coeffs, step, step_rows, base, rows, rho_refs, in_ref, prev_in_ref, prev_res_ref, s_refs, n_orig):
    rho_out = read_rows(rho_refs, step, step_rows, base, rows, me).astype(f32)
    here = pl.ds(base, rows)
    rho_in = in_ref[here, :]
    res = rho_out - rho_in
    newest = (rho_in - prev_in_ref[here, :]) + mixing_weight * (res - prev_res_ref[here, :])
    dens = rho_in + mixing_weight * res
    at = 0
    if n_orig:
        orig = s_refs[0]
        for j in range(n_orig):
            dens = dens - coeffs[at] * orig[DEPTH - 1 - n_orig + j, here, :].astype(f32)
            at += 1
    for ref in s_refs[1 if n_orig else 0 :]:
        dens = dens - coeffs[at] * ref[here, :].astype(f32)
        at += 1
    dens = dens - coeffs[at] * newest
    return dens, res, newest


def forward_kernel(kind, bands, planes, n_extra, n_orig, groups, cells, me_ref, *refs):
    refs = list(refs)
    take = lambda k: [refs.pop(0) for _ in range(k)]
    mixing = kind != "start"
    me = me_ref[0]
    if mixing:
        first = n_extra == 0
        (stats_ref,) = take(1)
        carry_ref = None if first else take(1)[0]
        rho_refs = take(2)
        in_ref, prev_in_ref, prev_res_ref = take(3)
        s_refs = take(1 + n_extra)
    else:
        (in_ref,) = take(1)
    if kind != "last":
        ext_ref, psi_ref, wz_ref, ly_ref = take(4)
        out_refs = take(groups)
    if mixing:
        dens_ref, res_ref = take(2)
        if kind == "mix":
            new_ref, carry_out = take(2)
        (coeff_ref,) = take(1)

        @pl.when(pl.program_id(0) == 0)
        def _():
            gram, rhs = finish_stats(stats_ref, carry_ref, first, cells)
            for j, c in enumerate(solve_rows(gram, rhs)):
                coeff_ref[j : j + 1, :] = c
            if kind == "mix":
                carry_out[...] = jnp.zeros_like(carry_out)
                for (j, k), i in pair_index(DEPTH - 1).items():
                    carry_out[i : i + 1, :] = gram[j + 1][k + 1]

        coeffs = [coeff_ref[j : j + 1, :] for j in range(DEPTH)]
    if kind != "last":
        (scratch,) = take(1)
        kept = ly_ref.shape[0] // 2
        sign = half_sign((kept, LANES), 1.0)
    for xi in range(planes):
        here = pl.ds(xi * LANES, LANES)
        if mixing:
            dens, res, newest = mix_plane(
                me, coeffs, pl.program_id(0), planes * LANES, xi * LANES, LANES,
                rho_refs, in_ref, prev_in_ref, prev_res_ref, s_refs, n_orig,
            )
            dens_ref[here, :] = dens
            res_ref[here, :] = res
            if kind == "mix":
                new_ref[here, :] = newest.astype(new_ref.dtype)
        else:
            dens = in_ref[here, :]
        if kind == "last":
            continue
        factor = jnp.exp(-time_step * (ext_ref[here, :] + dens - energy_shift))
        for b in range(bands):
            w = jnp.concatenate(
                [(psi_ref[c, b, xi].astype(f32) * factor).astype(bf16) for c in range(2)], axis=1
            )
            a = dot(w, wz_ref[...]).astype(bf16)
            t = dot(ly_ref[...], a)
            out = t[:kept] + sign * swap_halves(t[kept:])
            scratch[b, pl.ds(xi, kept, stride=planes), :] = out
    if kind != "last":
        per = kept // groups
        for b in range(bands):
            for g in range(groups):
                rows = scratch[b, pl.ds(g * per * planes, per * planes), :]
                out_refs[g][b] = rows.reshape(per, planes, LANES).astype(bf16)


def forward(kind, me, bands, slab, groups, cells, ext=None, psi=None, wz=None, ly=None,
            density=None, mix=None):
    planes = min(8, slab)
    steps = slab // planes
    block = planes * LANES
    rows = slab * LANES
    const2 = lambda shape: pl.BlockSpec(shape, lambda s, m: (0,) * len(shape))
    rowspec = pl.BlockSpec((block, LANES), lambda s, m: (s, 0))
    args, specs, outs, out_specs, scratch = [], [], [], [], []
    n_extra = n_orig = 0
    if kind != "start":
        n_extra = len(mix["extra"])
        n_orig = DEPTH - 1 - n_extra
        args.append(mix["stats"])
        specs.append(const2(mix["stats"].shape))
        if n_extra:
            args.append(mix["carry"])
            specs.append(const2(mix["carry"].shape))
        for r in mix["rho"]:
            args.append(r)
            specs.append(const2(r.shape))
        for v in (mix["rho_in"], mix["prev_in"], mix["prev_res"]):
            args.append(v)
            specs.append(rowspec)
        args.append(mix["orig"])
        specs.append(pl.BlockSpec((DEPTH - 1, block, LANES), lambda s, m: (0, s, 0)))
        for v in mix["extra"]:
            args.append(v)
            specs.append(rowspec)
    else:
        args.append(density)
        specs.append(rowspec)
    if kind != "last":
        kept = ly.shape[0] // 2
        per = kept // groups
        args += [ext, psi, wz, ly]
        specs += [
            rowspec,
            pl.BlockSpec((2, bands, planes, LANES, LANES), lambda s, m: (0, 0, s, 0, 0)),
            const2(wz.shape),
            const2(ly.shape),
        ]
        outs += [jax.ShapeDtypeStruct((bands, per, slab, LANES), bf16)] * groups
        out_specs += [pl.BlockSpec((bands, per, planes, LANES), lambda s, m: (0, 0, s, 0))] * groups
    if kind != "start":
        outs += [jax.ShapeDtypeStruct((rows, LANES), f32)] * 2
        out_specs += [rowspec] * 2
        if kind == "mix":
            outs += [jax.ShapeDtypeStruct((rows, LANES), bf16), jax.ShapeDtypeStruct((CARRY_ROWS, LANES), f32)]
            out_specs += [rowspec, const2((CARRY_ROWS, LANES))]
        scratch.append(pltpu.VMEM((8, LANES), f32))
    if kind != "last":
        scratch.append(pltpu.VMEM((bands, kept * planes, LANES), f32))
    return pl.pallas_call(
        functools.partial(forward_kernel, kind, bands, planes, n_extra, n_orig, groups, cells),
        grid_spec=pltpu.PrefetchScalarGridSpec(
            num_scalar_prefetch=1, grid=(steps,), in_specs=specs, out_specs=out_specs, scratch_shapes=scratch
        ),
        out_shape=outs,
        compiler_params=pltpu.CompilerParams(vmem_limit_bytes=40 << 20),
        cost_estimate=pl.CostEstimate(flops=3 * 10**9, bytes_accessed=16 << 20, transcendentals=0),
        name="forward_" + kind,
    )(me, *args)


def filter_kernel(groups, *refs):
    in_refs, refs = refs[:groups], refs[groups:]
    lf_ref, li_ref, kin_ref = refs[:3]
    out_refs = refs[3:]
    bands, per, slab, _ = in_refs[0].shape
    kept = lf_ref.shape[0] // 2
    fsign = half_sign((kept, LANES), 1.0)
    isign = half_sign((kept, LANES), -1.0)
    for b in range(bands):
        for k in range(per):
            a = jnp.concatenate([r[b, k] for r in in_refs], axis=0)
            t = dot(lf_ref[...], a)
            c = (t[:kept] + fsign * swap_halves(t[kept:])) * kin_ref[k]
            both = jnp.concatenate([c.astype(bf16), (isign * swap_halves(c)).astype(bf16)], axis=0)
            d = dot(li_ref[...], both).astype(bf16)
            for g in range(groups):
                out_refs[g][b, k] = d[g * slab : (g + 1) * slab]


def x_filter(blocks, lf, li, kinetic):
    groups = len(blocks)
    bands, per, slab, _ = blocks[0].shape
    split = 2 if per % 2 == 0 else 1
    spec = pl.BlockSpec((bands, per // split, slab, LANES), lambda s: (0, s, 0, 0))
    const = lambda v: pl.BlockSpec(v.shape, lambda s: (0,) * v.ndim)
    return pl.pallas_call(
        functools.partial(filter_kernel, groups),
        grid=(split,),
        in_specs=[spec] * groups
        + [const(lf), const(li), pl.BlockSpec((per // split,) + kinetic.shape[1:], lambda s: (s, 0, 0))],
        out_specs=[spec] * groups,
        out_shape=[jax.ShapeDtypeStruct(blocks[0].shape, bf16)] * groups,
        compiler_params=pltpu.CompilerParams(vmem_limit_bytes=24 << 20),
        cost_estimate=pl.CostEstimate(flops=10**9, bytes_accessed=3 << 20, transcendentals=0),
        name="x_filter",
    )(*blocks, lf, li, kinetic)


def inverse_kernel(groups, planes, scale, keep_psi, me_ref, *refs):
    in_refs, refs = refs[:groups], refs[groups:]
    occ_ref, liy_ref, wiz_ref = refs[:3]
    refs = refs[3:]
    if keep_psi:
        psi_ref, refs = refs[0], refs[1:]
    rho_refs, scratch = refs[:2], refs[2]
    me = me_ref[0]
    bands, per = in_refs[0].shape[:2]
    kept = per * groups
    isign = half_sign((kept, LANES), -1.0)
    for b in range(bands):
        for g in range(groups):
            scratch[b, pl.ds(g * per * planes, per * planes), :] = (
                in_refs[g][b].astype(f32).reshape(per * planes, LANES)
            )
    for xi in range(planes):
        total = None
        for b in range(bands):
            v = scratch[b, pl.ds(xi, kept, stride=planes), :]
            both = jnp.concatenate([v.astype(bf16), (isign * swap_halves(v)).astype(bf16)], axis=0)
            e = dot(liy_ref[...], both).astype(bf16)
            psi = dot(e, wiz_ref[...]).astype(bf16)
            re, im = psi[:, :LANES], psi[:, LANES:]
            if keep_psi:
                psi_ref[0, b, xi] = re
                psi_ref[1, b, xi] = im
            re, im = re.astype(f32), im.astype(f32)
            part = (occ_ref[b] * scale) * (re * re + im * im)
            total = part if total is None else total + part
        write_rows(rho_refs, pl.program_id(0), planes * LANES, xi * LANES, total.astype(bf16), me)


def inverse(me, blocks, occ, liy, wiz, band_devices, scale, keep_psi):
    groups = len(blocks)
    bands, per, slab, _ = blocks[0].shape
    planes = min(8, slab)
    half = slab * LANES // band_devices // 2
    spec = pl.BlockSpec((bands, per, planes, LANES), lambda s, m: (0, 0, s, 0))
    const = lambda shape: pl.BlockSpec(shape, lambda s, m: (0,) * len(shape))
    outs = [jax.ShapeDtypeStruct((band_devices, half, LANES), bf16)] * 2
    out_specs = [const(outs[0].shape)] * 2
    if keep_psi:
        outs = [jax.ShapeDtypeStruct((2, bands, slab, LANES, LANES), bf16)] + outs
        out_specs = [pl.BlockSpec((2, bands, planes, LANES, LANES), lambda s, m: (0, 0, s, 0, 0))] + out_specs
    return pl.pallas_call(
        functools.partial(inverse_kernel, groups, planes, scale, keep_psi),
        grid_spec=pltpu.PrefetchScalarGridSpec(
            num_scalar_prefetch=1,
            grid=(slab // planes,),
            in_specs=[spec] * groups
            + [pl.BlockSpec(memory_space=pltpu.SMEM), const(liy.shape), const(wiz.shape)],
            out_specs=out_specs,
            scratch_shapes=[pltpu.VMEM((bands, per * groups * planes, LANES), f32)],
        ),
        out_shape=outs,
        compiler_params=pltpu.CompilerParams(vmem_limit_bytes=24 << 20),
        cost_estimate=pl.CostEstimate(flops=3 * 10**9, bytes_accessed=8 << 20, transcendentals=0),
        name="inverse",
    )(me, *blocks, occ, liy, wiz)


def partner(v, axis, size, mask):
    return lax.ppermute(v, axis, [(i, i ^ mask) for i in range(size)])


def exchange(blocks, axis, size):
    if size > 4:
        index = lax.axis_index(axis)
        order = jnp.arange(size, dtype=jnp.int32) ^ index
        stacked = jnp.stack(blocks)[order]
        got = lax.all_to_all(stacked, axis, 0, 0)[order]
        return [got[m] for m in range(size)]
    return [blocks[0]] + [partner(blocks[m], axis, size, m) for m in range(1, size)]


def reduce_blocks(v, axis, size, order):
    bits = size.bit_length() - 1
    v = v.reshape((2,) * bits + v.shape[1:])
    live = list(reversed(range(bits)))
    for bit in order:
        at = live.index(bit)
        mine = lax.index_in_dim(v, 0, at, keepdims=False)
        theirs = lax.index_in_dim(v, 1, at, keepdims=False)
        got = partner(theirs, axis, size, 1 << bit)
        v = (mine.astype(f32) + got.astype(f32)).astype(bf16)
        live.pop(at)
    return v


def gather_blocks(v, axis, size, order):
    bits = size.bit_length() - 1
    shape = v.shape
    live = []
    for bit in order:
        at = sum(1 for other in live if other > bit)
        got = partner(v, axis, size, 1 << bit)
        v = jnp.stack([v, got], axis=at)
        live.append(bit)
    return v.reshape((size,) + shape)


def local(
    bands,
    occupations,
    external,
    density_in,
    prev_density,
    prev_residual,
    hist_density,
    hist_residual,
):
    groups = lax.axis_size("grid")
    band_devices = lax.axis_size("band")
    devices = groups * band_devices
    slab, ng = external.shape[:2]
    nbands = bands.shape[1]
    cells = float(ng) ** 3
    scale = density_scale / (occupations.shape[0] * band_devices)
    rows = slab * ng
    frequency = jnp.arange(-(ng // 4), ng // 4, dtype=jnp.int32)
    kept = frequency.shape[0]
    per = kept // groups
    cos, sin = fourier_tables(ng, frequency)
    grid_at = lax.axis_index("grid")
    relative = jnp.arange(groups, dtype=jnp.int32) ^ grid_at
    k_order = (relative[:, None] * per + jnp.arange(per, dtype=jnp.int32)[None, :]).reshape(-1)
    x_order = (relative[:, None] * slab + jnp.arange(slab, dtype=jnp.int32)[None, :]).reshape(-1)
    wz = jnp.concatenate(
        [jnp.concatenate([cos, -sin], axis=1), jnp.concatenate([sin, cos], axis=1)], axis=0
    )
    wiz = jnp.concatenate(
        [jnp.concatenate([cos.T, sin.T], axis=1), jnp.concatenate([-sin.T, cos.T], axis=1)], axis=0
    )
    cos_k, sin_k = cos[:, k_order], sin[:, k_order]
    cos_x, sin_x = cos[x_order], sin[x_order]
    ly = jnp.concatenate([cos_k.T, sin_k.T], axis=0)
    liy = jnp.concatenate([cos_k, sin_k], axis=1)
    lf = jnp.concatenate([cos_x.T, sin_x.T], axis=0)
    li = jnp.concatenate([cos_x, sin_x], axis=1)
    squared = (frequency * frequency).astype(f32)
    local_sq = lax.dynamic_slice_in_dim(squared, grid_at * per, per)
    quarter = ng / 4.0
    radius = local_sq[:, None, None] + squared[None, :, None] + jnp.tile(squared, 2)[None, None, :]
    kinetic = jnp.exp(-time_step * radius / (quarter * quarter))
    me = lax.axis_index("band").astype(jnp.int32).reshape(1)

    flat = lambda v: v.reshape(v.shape[:-3] + (rows, ng))
    ext, rho_in, prev_in, prev_res = map(flat, (external, density_in, prev_density, prev_residual))
    hist_r, hist_q = flat(hist_density), flat(hist_residual)
    bits = band_devices.bit_length() - 1
    order_a = list(range(bits))
    order_b = [1, 0] + list(range(2, bits))

    psi = bands
    prev_res_shard = prev_res
    extra = []
    new_q = []
    carry = None
    mix = None
    orig = combine(hist_r, hist_q, max(1, slab // 4))
    for iteration in range(ITERS):
        if iteration == 0:
            blocks = forward("start", me, nbands, slab, groups, cells, ext, psi, wz, ly, density=rho_in)
        else:
            out = forward("mix", me, nbands, slab, groups, cells, ext, psi, wz, ly, mix=mix)
            blocks = out[:groups]
            prev_in = rho_in
            rho_in, prev_res, newest_s, carry = out[groups:]
            extra = extra + [newest_s]
        blocks = exchange(blocks, "grid", groups)
        blocks = x_filter(blocks, lf, li, kinetic)
        blocks = exchange(blocks, "grid", groups)
        last = iteration == ITERS - 1
        out = inverse(me, blocks, occupations, liy, wiz, band_devices, scale, not last)
        if not last:
            psi, out = out[0], out[1:]
        part_a, part_b = out
        shard_a = reduce_blocks(part_a, "band", band_devices, order_a)
        shard_b = reduce_blocks(part_b, "band", band_devices, order_b)
        shard = jnp.concatenate([shard_a, shard_b], axis=0)
        rho_a = gather_blocks(shard_a, "band", band_devices, order_a[::-1])
        rho_b = gather_blocks(shard_b, "band", band_devices, order_b[::-1])
        if iteration == 0:
            residuals = hist_q
        else:
            n_old = DEPTH - 1 - len(new_q)
            residuals = [(hist_q, DEPTH - 1 - n_old + j) for j in range(n_old)] + new_q
        stats, newest_q, res_shard = dots(iteration == 0, me, shard, rho_in, prev_res_shard, residuals)
        new_q = new_q + [newest_q]
        prev_res_shard = res_shard
        gathered = lax.all_to_all(
            jnp.broadcast_to(stats[None], (devices,) + stats.shape), ("band", "grid"), 0, 0
        )
        mix = dict(stats=gathered, carry=carry, rho=(rho_a, rho_b), rho_in=rho_in, prev_in=prev_in,
                   prev_res=prev_res, orig=orig, extra=extra)
    density, residual = forward("last", me, nbands, slab, groups, cells, mix=mix)
    unflat = lambda v: v.reshape(slab, ng, ng)
    return unflat(density), unflat(residual)


def solution(mesh):
    placed = (
        P(None, "band", "grid", None, None),
        P("band"),
        P("grid", None, None),
        P("grid", None, None),
        P("grid", None, None),
        P("grid", None, None),
        P(None, "grid", None, None),
        P(None, "grid", None, None),
    )
    return jax.shard_map(
        local,
        mesh=mesh,
        in_specs=placed,
        out_specs=(P("grid", None, None), P("grid", None, None)),
        check_vma=False,
    )
```

```python
import functools
import math

import jax
import jax.numpy as jnp
from jax import lax
from jax.experimental import pallas as pl
from jax.experimental.pallas import tpu as pltpu
from jax.sharding import PartitionSpec as P

DEPTH = 6
ITERS = 3
LANES = 128

time_step = 0.25
energy_shift = 2.5
mixing_weight = 0.5
ridge_share = 0.1
ridge_floor = 0.01
density_scale = 8.0


f32 = jnp.float32
bf16 = jnp.bfloat16


def fourier_tables(length, frequency):
    positions = jnp.arange(length, dtype=jnp.int32)
    phase_index = positions[:, None] * frequency[None, :] % length
    angles = phase_index.astype(f32) * (2.0 * math.pi / length)
    unit_scale = 1.0 / math.sqrt(length)
    return (
        (jnp.cos(angles) * unit_scale).astype(bf16),
        (jnp.sin(angles) * unit_scale).astype(bf16),
    )


def dot(a, b):
    return jnp.dot(a, b, preferred_element_type=f32)


def swap_halves(v):
    return pltpu.roll(v, v.shape[-1] // 2, v.ndim - 1)


def half_sign(shape, first):
    lane = lax.broadcasted_iota(jnp.int32, shape, len(shape) - 1)
    return jnp.where(lane < shape[-1] // 2, first, -first).astype(f32)


def orders(devices):
    bits = devices.bit_length() - 1
    upper = list(range(bits))
    lower = ([1, 0] + upper[2:]) if bits > 1 else upper
    return upper, lower


def position(relative, order):
    out = None
    for i, bit in enumerate(order):
        part = lax.shift_left(lax.bitwise_and(lax.shift_right_logical(relative, bit), 1), len(order) - 1 - i)
        out = part if out is None else out + part
    return out


def units(half, devices, step, step_rows, row, count, me):
    assert step_rows % (2 * half) == 0
    unit = min(count, half)
    for at in range(0, count, unit):
        block, within = divmod(row + at, 2 * half)
        which, offset = divmod(within, half)
        relative = lax.bitwise_xor(step * (step_rows // (2 * half)) + block, me)
        yield which, position(relative, orders(devices)[which]), offset, at, unit


def read_rows(refs, step, step_rows, row, count, me):
    near, half = refs[0].shape[:2]
    out = []
    for which, at, offset, _, unit in units(half, 2 * near, step, step_rows, row, count, me):
        here = (lax.rem(at, near), pl.ds(offset, unit), slice(None))
        low, high = (refs[2 * which + i][here].astype(f32) for i in range(2))
        out.append(jnp.where(at < near, low, high))
    return out[0] if len(out) == 1 else jnp.concatenate(out, axis=0)


def write_rows(refs, step, step_rows, row, value, me):
    devices, half = refs[0].shape[:2]
    for which, to, offset, at, unit in units(half, devices, step, step_rows, row, value.shape[0], me):
        refs[which][to, pl.ds(offset, unit), :] = value[at : at + unit]


def solve_rows(gram, rhs):
    n = len(rhs)
    trace = gram[0][0]
    for j in range(1, n):
        trace = trace + gram[j][j]
    ridge = ridge_share * trace / n + ridge_floor
    a = [[gram[j][k] + ridge if j == k else gram[j][k] for k in range(n)] for j in range(n)]
    low = [[None] * n for _ in range(n)]
    diag = [None] * n
    inv = [None] * n
    for j in range(n):
        value = a[j][j]
        scaled = []
        for k in range(j):
            s = low[j][k] * diag[k]
            scaled.append(s)
            value = value - low[j][k] * s
        diag[j] = value
        inv[j] = 1.0 / value
        for r in range(j + 1, n):
            e = a[r][j]
            for k in range(j):
                e = e - low[r][k] * scaled[k]
            low[r][j] = e * inv[j]
    mid = []
    for j in range(n):
        e = rhs[j]
        for k in range(j):
            e = e - low[j][k] * mid[k]
        mid.append(e)
    out = [None] * n
    for j in reversed(range(n)):
        e = mid[j] * inv[j]
        for k in range(j + 1, n):
            e = e - low[k][j] * out[k]
        out[j] = e
    return out


def pair_index(n):
    return {(j, k): i for i, (j, k) in enumerate((j, k) for j in range(n) for k in range(j, n))}


STAT_ROWS = 32


def spread_diagonal(row):
    shape = (STAT_ROWS, LANES)
    lane = lax.broadcasted_iota(jnp.int32, shape, 1)
    own = lax.broadcasted_iota(jnp.int32, shape, 0)
    picked = jnp.where(lane == own, jnp.broadcast_to(row, shape), 0.0)
    return jnp.broadcast_to(jnp.sum(picked, axis=1, keepdims=True), shape)


def finish_stats(stats_ref, carry_ref, first, cells):
    total = stats_ref[0]
    for d in range(1, stats_ref.shape[0]):
        total = total + stats_ref[d]
    total = spread_diagonal(total * (1.0 / cells))
    n = DEPTH
    gram = [[None] * n for _ in range(n)]
    kept = pair_index(n - 1)
    for (j, k), i in kept.items():
        value = total[2 * n + i : 2 * n + i + 1] if first else carry_ref[i : i + 1, :]
        gram[j][k] = value
        gram[k][j] = value
    for j in range(n):
        value = total[j : j + 1]
        gram[j][n - 1] = value
        gram[n - 1][j] = value
    rhs = [total[n + j : n + j + 1] for j in range(n)]
    return gram, rhs


CARRY_ROWS = 16


def combine_kernel(r_ref, q_ref, s_ref):
    s_ref[...] = (r_ref[...] + mixing_weight * q_ref[...]).astype(s_ref.dtype)


def combine(hist_density, hist_residual, parts):
    depth, rows, lanes = hist_density.shape
    block = rows // parts
    spec = pl.BlockSpec((depth, block, lanes), lambda s: (0, s, 0))
    return pl.pallas_call(
        combine_kernel,
        grid=(parts,),
        in_specs=[spec, spec],
        out_specs=spec,
        out_shape=jax.ShapeDtypeStruct((depth, rows, lanes), bf16),
        compiler_params=pltpu.CompilerParams(vmem_limit_bytes=24 << 20),
        cost_estimate=pl.CostEstimate(
            flops=rows * lanes * depth * 200, bytes_accessed=rows * lanes * depth * 10, transcendentals=0
        ),
        name="combine",
    )(hist_density, hist_residual)


def row_sum(v):
    return jnp.sum(v, axis=0, keepdims=True)


def dots_kernel(first, me_ref, *refs):
    q_count = DEPTH - 1
    rho_ref, in_ref, prev_ref = refs[:3]
    refs = refs[3:]
    if first:
        hist_ref = refs[0]
        refs = refs[1:]
        q = [hist_ref[j] for j in range(q_count)]
    else:
        q = [refs[j][...] for j in range(q_count)]
        refs = refs[q_count:]
    stats_ref, newest_ref, res_ref = refs
    res = rho_ref[...].astype(f32) - in_ref[...]
    newest = res - prev_ref[...]
    newest_ref[...] = newest
    res_ref[...] = res
    rows = [row_sum(v * newest) for v in q] + [row_sum(newest * newest)]
    rows += [row_sum(v * res) for v in q] + [row_sum(newest * res)]
    if first:
        for j, k in pair_index(q_count):
            rows.append(row_sum(q[j] * q[k]))
    rows += [jnp.zeros((1, LANES), f32)] * (STAT_ROWS - len(rows))
    table = jnp.sum(jnp.concatenate(rows, axis=0), axis=1, keepdims=True)
    shape = (STAT_ROWS, LANES)
    lane = lax.broadcasted_iota(jnp.int32, shape, 1)
    own = lax.broadcasted_iota(jnp.int32, shape, 0)
    packed = row_sum(jnp.where(lane == own, jnp.broadcast_to(table, shape), 0.0))
    stats_ref[...] = jnp.broadcast_to(packed[None], stats_ref.shape)


def dots(first, me, devices, rho_shard, rho_in, prev_res, residuals):
    block = rho_shard.shape[0]
    mine = pl.BlockSpec((block, LANES), lambda s, m: (m[0], 0))
    whole = pl.BlockSpec((block, LANES), lambda s, m: (0, 0))
    if first:
        hist = [residuals]
        hist_specs = [pl.BlockSpec((DEPTH - 1, block, LANES), lambda s, m: (0, m[0], 0))]
    else:
        hist = list(residuals)
        hist_specs = [
            pl.BlockSpec((None, block, LANES), functools.partial(lambda j, s, m: (j, m[0], 0), r[1]))
            if isinstance(r, tuple)
            else whole
            for r in hist
        ]
        hist = [r[0] if isinstance(r, tuple) else r for r in hist]
    return pl.pallas_call(
        functools.partial(dots_kernel, first),
        grid_spec=pltpu.PrefetchScalarGridSpec(
            num_scalar_prefetch=1,
            grid=(1,),
            in_specs=[whole, mine, mine if first else whole] + hist_specs,
            out_specs=[
                pl.BlockSpec((devices, 1, LANES), lambda s, m: (0, 0, 0)),
                whole,
                whole,
            ],
        ),
        out_shape=[
            jax.ShapeDtypeStruct((devices, 1, LANES), f32),
            jax.ShapeDtypeStruct((block, LANES), f32),
            jax.ShapeDtypeStruct((block, LANES), f32),
        ],
        compiler_params=pltpu.CompilerParams(vmem_limit_bytes=16 << 20),
        cost_estimate=pl.CostEstimate(flops=10**7, bytes_accessed=block * LANES * 32, transcendentals=0),
        name="dots",
    )(me, rho_shard, rho_in, prev_res, *hist)


def mix_plane(me, coeffs, step, step_rows, base, rows, rho_refs, in_ref, prev_in_ref, prev_res_ref, s_refs):
    rho_out = read_rows(rho_refs, step, step_rows, base, rows, me).astype(f32)
    here = pl.ds(base, rows)
    rho_in = in_ref[here, :]
    res = rho_out - rho_in
    newest = (rho_in - prev_in_ref[here, :]) + mixing_weight * (res - prev_res_ref[here, :])
    dens = rho_in + mixing_weight * res
    for c, ref in zip(coeffs, s_refs):
        dens = dens - c * ref[here, :].astype(f32)
    dens = dens - coeffs[-1] * newest
    return dens, res, newest


def forward_kernel(kind, planes, first, groups, cells, me_ref, *refs):
    refs = list(refs)
    take = lambda k: [refs.pop(0) for _ in range(k)]
    mixing = kind != "plain"
    me = me_ref[0]
    if mixing:
        (stats_ref,) = take(1)
        carry_ref = None if first else take(1)[0]
        rho_refs = take(4)
        in_ref, prev_in_ref, prev_res_ref = take(3)
        s_refs = take(DEPTH - 1)
    else:
        (in_ref,) = take(1)
    if kind != "last":
        ext_ref, psi_ref, wz_ref, ly_ref = take(4)
        out_refs = take(groups)
    if mixing:
        dens_ref, res_ref = take(2)
        if kind == "mix":
            new_ref, carry_out = take(2)
        (coeff_ref,) = take(1)

        @pl.when(pl.program_id(0) == 0)
        def _():
            gram, rhs = finish_stats(stats_ref, carry_ref, first, cells)
            for j, c in enumerate(solve_rows(gram, rhs)):
                coeff_ref[j : j + 1, :] = c
            if kind == "mix":
                carry_out[...] = jnp.zeros_like(carry_out)
                for (j, k), i in pair_index(DEPTH - 1).items():
                    carry_out[i : i + 1, :] = gram[j + 1][k + 1]

        coeffs = [coeff_ref[j : j + 1, :] for j in range(DEPTH)]
    if kind != "last":
        w_ref, a_ref, scratch = take(3)
    for xi in range(planes):
        here = pl.ds(xi * LANES, LANES)
        if mixing:
            dens, res, newest = mix_plane(
                me, coeffs, pl.program_id(0), planes * LANES, xi * LANES, LANES,
                rho_refs, in_ref, prev_in_ref, prev_res_ref, s_refs,
            )
            dens_ref[here, :] = dens
            res_ref[here, :] = res
            if kind == "mix":
                new_ref[here, :] = newest.astype(new_ref.dtype)
        else:
            dens = in_ref[here, :]
        if kind != "last":
            factor = jnp.exp(-time_step * (ext_ref[here, :] + dens - energy_shift))
            for c in range(2):
                w_ref[here, c * LANES : (c + 1) * LANES] = (psi_ref[c, xi].astype(f32) * factor).astype(bf16)
    if kind == "last":
        return
    kept = ly_ref.shape[0] // 2
    sign = half_sign((kept, LANES), 1.0)
    a_ref[...] = dot(w_ref[...], wz_ref[...]).astype(bf16)
    for pair in pairs(planes):
        wide = [a_ref[xi * LANES : (xi + 1) * LANES, :] for xi in pair]
        t = dot(ly_ref[...], jnp.concatenate(wide, axis=1))
        for i, xi in enumerate(pair):
            lanes = slice(i * LANES, (i + 1) * LANES)
            out = t[:kept, lanes] + sign * swap_halves(t[kept:, lanes])
            scratch[pl.ds(xi, kept, stride=planes), :] = out
    per = kept // groups
    for g in range(groups):
        rows = scratch[g * per * planes : (g + 1) * per * planes, :]
        out_refs[g][...] = rows.reshape(per, planes, LANES).astype(bf16)


def pairs(count):
    return [tuple(range(i, min(i + 2, count))) for i in range(0, count, 2)]


def forward(kind, me, slab, groups, cells, ext=None, psi=None, band=0, wz=None, ly=None, density=None, mix=None):
    planes = min(8, slab)
    steps = slab // planes
    block = planes * LANES
    rows = slab * LANES
    const = lambda shape: pl.BlockSpec(shape, lambda s, m: (0,) * len(shape))
    rowspec = pl.BlockSpec((block, LANES), lambda s, m: (s, 0))
    args, specs, outs, out_specs, scratch = [], [], [], [], []
    first = False
    if kind != "plain":
        first = mix["carry"] is None
        small = [mix["stats"]] + ([] if first else [mix["carry"]]) + list(mix["rho"])
        args += small
        specs += [const(v.shape) for v in small]
        args += [mix["rho_in"], mix["prev_in"], mix["prev_res"]]
        specs += [rowspec] * 3
        extra = mix["extra"]
        for j in range(len(extra), DEPTH - 1):
            args.append(mix["orig"])
            specs.append(pl.BlockSpec((None, block, LANES), functools.partial(lambda j, s, m: (j, s, 0), j)))
        args += extra
        specs += [rowspec] * len(extra)
    else:
        args.append(density)
        specs.append(rowspec)
    if kind != "last":
        kept = ly.shape[0] // 2
        per = kept // groups
        args += [ext, psi, wz, ly]
        specs += [
            rowspec,
            pl.BlockSpec((2, None, planes, LANES, LANES), lambda s, m: (0, band, s, 0, 0)),
            const(wz.shape),
            const(ly.shape),
        ]
        outs += [jax.ShapeDtypeStruct((per, slab, LANES), bf16)] * groups
        out_specs += [pl.BlockSpec((per, planes, LANES), lambda s, m: (0, s, 0))] * groups
    if kind != "plain":
        outs += [jax.ShapeDtypeStruct((rows, LANES), f32)] * 2
        out_specs += [rowspec] * 2
        if kind == "mix":
            outs += [jax.ShapeDtypeStruct((rows, LANES), bf16), jax.ShapeDtypeStruct((CARRY_ROWS, LANES), f32)]
            out_specs += [rowspec, const((CARRY_ROWS, LANES))]
        scratch.append(pltpu.VMEM((8, LANES), f32))
    if kind != "last":
        scratch += [
            pltpu.VMEM((block, 2 * LANES), bf16),
            pltpu.VMEM((block, LANES), bf16),
            pltpu.VMEM((kept * planes, LANES), f32),
        ]
    return pl.pallas_call(
        functools.partial(forward_kernel, kind, planes, first, groups, cells),
        grid_spec=pltpu.PrefetchScalarGridSpec(
            num_scalar_prefetch=1, grid=(steps,), in_specs=specs, out_specs=out_specs, scratch_shapes=scratch
        ),
        out_shape=outs,
        compiler_params=pltpu.CompilerParams(vmem_limit_bytes=20 << 20),
        cost_estimate=pl.CostEstimate(flops=10**9, bytes_accessed=6 << 20, transcendentals=0),
        name="forward_" + kind,
    )(me, *args)


def filter_kernel(groups, *refs):
    in_refs, refs = refs[:groups], refs[groups:]
    lf_ref, li_ref, kin_ref = refs[:3]
    out_refs = refs[3:]
    per, slab, _ = in_refs[0].shape
    kept = lf_ref.shape[0] // 2
    fsign = half_sign((kept, LANES), 1.0)
    isign = half_sign((kept, LANES), -1.0)
    for pair in pairs(per):
        wide = [jnp.concatenate([r[k] for r in in_refs], axis=0) for k in pair]
        t = dot(lf_ref[...], jnp.concatenate(wide, axis=1))
        both = []
        for i, k in enumerate(pair):
            lanes = slice(i * LANES, (i + 1) * LANES)
            c = (t[:kept, lanes] + fsign * swap_halves(t[kept:, lanes])) * kin_ref[k]
            both.append(jnp.concatenate([c.astype(bf16), (isign * swap_halves(c)).astype(bf16)], axis=0))
        d = dot(li_ref[...], jnp.concatenate(both, axis=1)).astype(bf16)
        for i, k in enumerate(pair):
            for g in range(groups):
                out_refs[g][k] = d[g * slab : (g + 1) * slab, i * LANES : (i + 1) * LANES]


def x_filter(blocks, lf, li, kinetic):
    groups = len(blocks)
    per, slab, _ = blocks[0].shape
    split = 2 if per % 4 == 0 else 1
    spec = pl.BlockSpec((per // split, slab, LANES), lambda s: (s, 0, 0))
    const = lambda v: pl.BlockSpec(v.shape, lambda s: (0,) * v.ndim)
    return pl.pallas_call(
        functools.partial(filter_kernel, groups),
        grid=(split,),
        in_specs=[spec] * groups
        + [const(lf), const(li), pl.BlockSpec((per // split,) + kinetic.shape[1:], lambda s: (s, 0, 0))],
        out_specs=[spec] * groups,
        out_shape=[jax.ShapeDtypeStruct(blocks[0].shape, bf16)] * groups,
        compiler_params=pltpu.CompilerParams(vmem_limit_bytes=12 << 20),
        cost_estimate=pl.CostEstimate(flops=5 * 10**8, bytes_accessed=2 << 20, transcendentals=0),
        name="x_filter",
    )(*blocks, lf, li, kinetic)


def inverse_kernel(groups, planes, scale, band, adds, ends, keep_psi, me_ref, *refs):
    in_refs, refs = refs[:groups], refs[groups:]
    occ_ref, liy_ref, wiz_ref = refs[:3]
    refs = list(refs[3:])
    if adds:
        part_ref = refs.pop(0)
    if keep_psi:
        psi_ref = refs.pop(0)
    if ends:
        rho_refs = [refs.pop(0) for _ in range(2)]
    else:
        total_ref = refs.pop(0)
    scratch, e_ref = refs
    me = me_ref[0]
    per = in_refs[0].shape[0]
    kept = per * groups
    isign = half_sign((kept, LANES), -1.0)
    for g in range(groups):
        scratch[g * per * planes : (g + 1) * per * planes, :] = (
            in_refs[g][...].astype(f32).reshape(per * planes, LANES)
        )
    for pair in pairs(planes):
        both = []
        for xi in pair:
            v = scratch[pl.ds(xi, kept, stride=planes), :]
            both.append(jnp.concatenate([v.astype(bf16), (isign * swap_halves(v)).astype(bf16)], axis=0))
        e = dot(liy_ref[...], jnp.concatenate(both, axis=1)).astype(bf16)
        for i, xi in enumerate(pair):
            e_ref[xi * LANES : (xi + 1) * LANES, :] = e[:, i * LANES : (i + 1) * LANES]
    for xi in range(planes):
        here = pl.ds(xi * LANES, LANES)
        psi = dot(e_ref[here, :], wiz_ref[...]).astype(bf16)
        re, im = psi[:, :LANES], psi[:, LANES:]
        if keep_psi:
            psi_ref[0, xi] = re
            psi_ref[1, xi] = im
        re, im = re.astype(f32), im.astype(f32)
        total = (occ_ref[band] * scale) * (re * re + im * im)
        if adds:
            total = total + part_ref[here, :]
        if ends:
            write_rows(rho_refs, pl.program_id(0), planes * LANES, xi * LANES, total.astype(bf16), me)
        else:
            total_ref[here, :] = total


def inverse(me, blocks, occ, band, bands, liy, wiz, band_devices, scale, keep_psi, part):
    groups = len(blocks)
    per, slab, _ = blocks[0].shape
    planes = min(8, slab)
    rows, block = slab * LANES, planes * LANES
    half = rows // band_devices // 2
    adds, ends = part is not None, band == bands - 1
    spec = pl.BlockSpec((per, planes, LANES), lambda s, m: (0, s, 0))
    rowspec = pl.BlockSpec((block, LANES), lambda s, m: (s, 0))
    const = lambda shape: pl.BlockSpec(shape, lambda s, m: (0,) * len(shape))
    outs, out_specs = [], []
    if keep_psi:
        outs.append(jax.ShapeDtypeStruct((2, 1, slab, LANES, LANES), bf16))
        out_specs.append(pl.BlockSpec((2, None, planes, LANES, LANES), lambda s, m: (0, 0, s, 0, 0)))
    if ends:
        outs += [jax.ShapeDtypeStruct((band_devices, half, LANES), bf16)] * 2
        out_specs += [const(outs[-1].shape)] * 2
    else:
        outs.append(jax.ShapeDtypeStruct((rows, LANES), f32))
        out_specs.append(rowspec)
    return pl.pallas_call(
        functools.partial(inverse_kernel, groups, planes, scale, band, adds, ends, keep_psi),
        grid_spec=pltpu.PrefetchScalarGridSpec(
            num_scalar_prefetch=1,
            grid=(slab // planes,),
            in_specs=[spec] * groups
            + [pl.BlockSpec(memory_space=pltpu.SMEM), const(liy.shape), const(wiz.shape)]
            + ([rowspec] if adds else []),
            out_specs=out_specs,
            scratch_shapes=[
                pltpu.VMEM((per * groups * planes, LANES), f32),
                pltpu.VMEM((block, LANES), bf16),
            ],
        ),
        out_shape=outs,
        compiler_params=pltpu.CompilerParams(vmem_limit_bytes=16 << 20),
        cost_estimate=pl.CostEstimate(flops=10**9, bytes_accessed=4 << 20, transcendentals=0),
        name="inverse",
    )(me, *blocks, occ, liy, wiz, *([part] if adds else []))


def partner(v, axis, size, mask):
    return lax.ppermute(v, axis, [(i, i ^ mask) for i in range(size)])


def exchange(blocks, axis, size):
    if size > 4:
        index = lax.axis_index(axis)
        order = jnp.arange(size, dtype=jnp.int32) ^ index
        stacked = jnp.stack(blocks)[order]
        got = lax.all_to_all(stacked, axis, 0, 0)[order]
        return [got[m] for m in range(size)]
    return [blocks[0]] + [partner(blocks[m], axis, size, m) for m in range(1, size)]


def reduce_blocks(v, axis, size, order):
    for bit in order:
        half = v.shape[0] // 2
        got = partner(v[half:], axis, size, 1 << bit)
        v = (v[:half].astype(f32) + got.astype(f32)).astype(bf16)
    return v


def gather_blocks(v, axis, size, order):
    for i, bit in enumerate(reversed(order)):
        got = partner(v, axis, size, 1 << bit)
        if i == len(order) - 1:
            return v, got
        v = jnp.concatenate([v, got], axis=0)


def local(
    bands,
    occupations,
    external,
    density_in,
    prev_density,
    prev_residual,
    hist_density,
    hist_residual,
):
    groups = lax.axis_size("grid")
    band_devices = lax.axis_size("band")
    devices = groups * band_devices
    slab, ng = external.shape[:2]
    nbands = bands.shape[1]
    cells = float(ng) ** 3
    scale = density_scale / (occupations.shape[0] * band_devices)
    rows = slab * ng
    frequency = jnp.arange(-(ng // 4), ng // 4, dtype=jnp.int32)
    kept = frequency.shape[0]
    per = kept // groups
    cos, sin = fourier_tables(ng, frequency)
    grid_at = lax.axis_index("grid")
    relative = jnp.arange(groups, dtype=jnp.int32) ^ grid_at
    k_order = (relative[:, None] * per + jnp.arange(per, dtype=jnp.int32)[None, :]).reshape(-1)
    x_order = (relative[:, None] * slab + jnp.arange(slab, dtype=jnp.int32)[None, :]).reshape(-1)
    wz = jnp.concatenate(
        [jnp.concatenate([cos, -sin], axis=1), jnp.concatenate([sin, cos], axis=1)], axis=0
    )
    wiz = jnp.concatenate(
        [jnp.concatenate([cos.T, sin.T], axis=1), jnp.concatenate([-sin.T, cos.T], axis=1)], axis=0
    )
    cos_k, sin_k = cos[:, k_order], sin[:, k_order]
    cos_x, sin_x = cos[x_order], sin[x_order]
    ly = jnp.concatenate([cos_k.T, sin_k.T], axis=0)
    liy = jnp.concatenate([cos_k, sin_k], axis=1)
    lf = jnp.concatenate([cos_x.T, sin_x.T], axis=0)
    li = jnp.concatenate([cos_x, sin_x], axis=1)
    squared = (frequency * frequency).astype(f32)
    local_sq = lax.dynamic_slice_in_dim(squared, grid_at * per, per)
    quarter = ng / 4.0
    radius = local_sq[:, None, None] + squared[None, :, None] + jnp.tile(squared, 2)[None, None, :]
    kinetic = jnp.exp(-time_step * radius / (quarter * quarter))
    me = lax.axis_index("band").astype(jnp.int32).reshape(1)

    flat = lambda v: v.reshape(v.shape[:-3] + (rows, ng))
    ext, rho_in, prev_in, prev_res = map(flat, (external, density_in, prev_density, prev_residual))
    hist_r, hist_q = flat(hist_density), flat(hist_residual)
    upper, lower = orders(band_devices)
    psi = [(bands, b) for b in range(nbands)]
    prev_res_shard = prev_res
    extra = []
    new_q = []
    carry = None
    mix = None
    orig = combine(hist_r, hist_q, max(1, slab // 4))
    common = dict(ext=ext, wz=wz, ly=ly)
    for iteration in range(ITERS):
        blocks = []
        for b, (array, at) in enumerate(psi):
            if iteration and b == 0:
                out = forward("mix", me, slab, groups, cells, psi=array, band=at, mix=mix, **common)
                prev_in = rho_in
                rho_in, prev_res, newest_s, carry = out[groups:]
                extra = extra + [newest_s]
            else:
                out = forward("plain", me, slab, groups, cells, psi=array, band=at, density=rho_in, **common)
            blocks.append(exchange(out[:groups], "grid", groups))
        if iteration == 0:
            blocks[-1], orig = lax.optimization_barrier((blocks[-1], orig))
        for b in range(nbands):
            blocks[b] = exchange(x_filter(blocks[b], lf, li, kinetic), "grid", groups)
        last = iteration == ITERS - 1
        part = None
        psi = []
        for b in range(nbands):
            out = inverse(
                me, blocks[b], occupations, b, nbands, liy, wiz, band_devices, scale, not last, part
            )
            if not last:
                psi.append((out[0], 0))
                out = out[1:]
            part = out[0]
        shard_a = reduce_blocks(out[0], "band", band_devices, upper)
        shard_b = reduce_blocks(out[1], "band", band_devices, lower)
        shard = jnp.concatenate([shard_a[0], shard_b[0]], axis=0)
        rho = gather_blocks(shard_a, "band", band_devices, upper) + gather_blocks(
            shard_b, "band", band_devices, lower
        )
        if iteration == 0:
            residuals = hist_q
        else:
            n_old = DEPTH - 1 - len(new_q)
            residuals = [(hist_q, DEPTH - 1 - n_old + j) for j in range(n_old)] + new_q
        stats, newest_q, prev_res_shard = dots(
            iteration == 0, me, devices, shard, rho_in, prev_res_shard, residuals
        )
        new_q = new_q + [newest_q]
        gathered = lax.all_to_all(stats, ("band", "grid"), 0, 0)
        mix = dict(stats=gathered, carry=carry, rho=rho, rho_in=rho_in, prev_in=prev_in,
                   prev_res=prev_res, orig=orig, extra=extra)
    density, residual = forward("last", me, slab, groups, cells, mix=mix)
    unflat = lambda v: v.reshape(slab, ng, ng)
    return unflat(density), unflat(residual)


def solution(mesh):
    placed = (
        P(None, "band", "grid", None, None),
        P("band"),
        P("grid", None, None),
        P("grid", None, None),
        P("grid", None, None),
        P("grid", None, None),
        P(None, "grid", None, None),
        P(None, "grid", None, None),
    )
    return jax.shard_map(
        local,
        mesh=mesh,
        in_specs=placed,
        out_specs=(P("grid", None, None), P("grid", None, None)),
        check_vma=False,
    )
```

```python
import functools
import math

import jax
import jax.numpy as jnp
import ml_dtypes
import numpy as np
from jax import lax
from jax.experimental import pallas as pl
from jax.experimental.pallas import tpu as pltpu
from jax.sharding import PartitionSpec as P

DEPTH = 6
ITERS = 3
LANES = 128
PLANES = 16
FILTER_STEPS = 2

time_step = 0.25
energy_shift = 2.5
mixing_weight = 0.5
ridge_share = 0.1
ridge_floor = 0.01
density_scale = 8.0


f32 = jnp.float32
bf16 = jnp.bfloat16


def fourier_tables(length, groups):
    frequency = np.arange(-(length // 4), length // 4)
    phase_index = np.arange(length)[:, None] * frequency[None, :] % length
    angles = phase_index.astype(np.float32) * np.float32(2.0 * math.pi / length)
    unit_scale = np.float32(1.0 / math.sqrt(length))
    cos, sin = (f(angles).astype(np.float32) * unit_scale for f in (np.cos, np.sin))
    out = [
        np.block([[cos, -sin], [sin, cos]]),
        np.block([[cos.T, sin.T], [-sin.T, cos.T]]),
    ]
    stacks = [[], [], [], []]
    for index in range(groups):
        def ordered(count):
            return np.concatenate([np.arange(count // groups) + (index ^ m) * (count // groups) for m in range(groups)])
        ck, sk = (v[:, ordered(len(frequency))] for v in (cos, sin))
        cx, sx = (v[ordered(length)] for v in (cos, sin))
        stacks[0].append(np.concatenate([ck.T, sk.T], axis=0))
        stacks[1].append(np.concatenate([ck, sk], axis=1))
        stacks[2].append(np.concatenate([cx.T, sx.T], axis=0))
        stacks[3].append(np.concatenate([cx, sx], axis=1))
    return [jnp.asarray(v.astype(ml_dtypes.bfloat16)) for v in out + [np.stack(v) for v in stacks]]


def dot(a, b):
    return jnp.dot(a, b, preferred_element_type=f32)


def swap_halves(v):
    return pltpu.roll(v, v.shape[-1] // 2, v.ndim - 1)


def half_sign(shape, first):
    lane = lax.broadcasted_iota(jnp.int32, shape, len(shape) - 1)
    return jnp.where(lane < shape[-1] // 2, first, -first).astype(f32)


def orders(devices):
    bits = devices.bit_length() - 1
    upper = list(range(bits))
    lower = ([1, 0] + upper[2:]) if bits > 1 else upper
    return upper, lower


def position(relative, order):
    out = None
    for i, bit in enumerate(order):
        part = lax.shift_left(lax.bitwise_and(lax.shift_right_logical(relative, bit), 1), len(order) - 1 - i)
        out = part if out is None else out + part
    return out


def units(half, devices, step, step_rows, row, count, me):
    assert step_rows % (2 * half) == 0
    unit = min(count, half)
    for at in range(0, count, unit):
        block, within = divmod(row + at, 2 * half)
        which, offset = divmod(within, half)
        relative = lax.bitwise_xor(step * (step_rows // (2 * half)) + block, me)
        yield which, position(relative, orders(devices)[which]), offset, at, unit


def read_rows(refs, step, step_rows, row, count, me):
    near, half = refs[0].shape[:2]
    out = []
    for which, at, offset, _, unit in units(half, 2 * near, step, step_rows, row, count, me):
        here = (lax.rem(at, near), pl.ds(offset, unit), slice(None))
        low, high = (refs[2 * which + i][here].astype(f32) for i in range(2))
        out.append(jnp.where(at < near, low, high))
    return out[0] if len(out) == 1 else jnp.concatenate(out, axis=0)


def write_rows(refs, step, step_rows, row, value, me):
    devices, half = refs[0].shape[:2]
    for which, to, offset, at, unit in units(half, devices, step, step_rows, row, value.shape[0], me):
        refs[which][to, pl.ds(offset, unit), :] = value[at : at + unit]


def solve_rows(gram, rhs):
    n = len(rhs)
    trace = gram[0][0]
    for j in range(1, n):
        trace = trace + gram[j][j]
    ridge = ridge_share * trace / n + ridge_floor
    a = [[gram[j][k] + ridge if j == k else gram[j][k] for k in range(n)] for j in range(n)]
    low = [[None] * n for _ in range(n)]
    diag = [None] * n
    inv = [None] * n
    for j in range(n):
        value = a[j][j]
        scaled = []
        for k in range(j):
            s = low[j][k] * diag[k]
            scaled.append(s)
            value = value - low[j][k] * s
        diag[j] = value
        inv[j] = 1.0 / value
        for r in range(j + 1, n):
            e = a[r][j]
            for k in range(j):
                e = e - low[r][k] * scaled[k]
            low[r][j] = e * inv[j]
    mid = []
    for j in range(n):
        e = rhs[j]
        for k in range(j):
            e = e - low[j][k] * mid[k]
        mid.append(e)
    out = [None] * n
    for j in reversed(range(n)):
        e = mid[j] * inv[j]
        for k in range(j + 1, n):
            e = e - low[k][j] * out[k]
        out[j] = e
    return out


def pair_index(n):
    return {(j, k): i for i, (j, k) in enumerate((j, k) for j in range(n) for k in range(j, n))}


STAT_ROWS = 32


def spread_diagonal(row):
    shape = (STAT_ROWS, LANES)
    lane = lax.broadcasted_iota(jnp.int32, shape, 1)
    own = lax.broadcasted_iota(jnp.int32, shape, 0)
    picked = jnp.where(lane == own, jnp.broadcast_to(row, shape), 0.0)
    return jnp.broadcast_to(jnp.sum(picked, axis=1, keepdims=True), shape)


def finish_stats(stats_ref, carry_ref, first, cells):
    total = spread_diagonal(stats_ref[...] * (1.0 / cells))
    n = DEPTH
    gram = [[None] * n for _ in range(n)]
    kept = pair_index(n - 1)
    for (j, k), i in kept.items():
        value = total[2 * n + i : 2 * n + i + 1] if first else carry_ref[i : i + 1, :]
        gram[j][k] = value
        gram[k][j] = value
    for j in range(n):
        value = total[j : j + 1]
        gram[j][n - 1] = value
        gram[n - 1][j] = value
    rhs = [total[n + j : n + j + 1] for j in range(n)]
    return gram, rhs


CARRY_ROWS = 16


def combine_kernel(tie_ref, r_ref, q_ref, s_ref):
    s_ref[...] = (r_ref[...] + mixing_weight * q_ref[...]).astype(s_ref.dtype)


def combine(tie, hist_density, hist_residual, j, parts):
    _, rows, lanes = hist_density.shape
    block = rows // parts
    spec = pl.BlockSpec((None, block, lanes), lambda s, t: (j, s, 0))
    return pl.pallas_call(
        combine_kernel,
        grid_spec=pltpu.PrefetchScalarGridSpec(
            num_scalar_prefetch=1,
            grid=(parts,),
            in_specs=[spec, spec],
            out_specs=pl.BlockSpec((block, lanes), lambda s, t: (s, 0)),
        ),
        out_shape=jax.ShapeDtypeStruct((rows, lanes), bf16),
        compiler_params=pltpu.CompilerParams(vmem_limit_bytes=12 << 20),
        cost_estimate=pl.CostEstimate(flops=10**8, bytes_accessed=rows * lanes * 10, transcendentals=0),
        name="combine",
    )(tie, hist_density, hist_residual)


def middle_kernel(me_ref, *refs):
    rho_refs, (in_ref, prev_ref, mid_ref, new_ref) = refs[:4], refs[4:]
    rows = in_ref.shape[0]
    for base in range(0, rows, LANES):
        here = pl.ds(base, LANES)
        rho_out = read_rows(rho_refs, pl.program_id(0), rows, base, LANES, me_ref[0])
        mid = mixing_weight * (rho_out + in_ref[here, :])
        mid_ref[here, :] = mid
        new_ref[here, :] = (mid - prev_ref[here, :]).astype(new_ref.dtype)


def middle(me, slab, rho, rho_in, prev_mid):
    planes = min(PLANES, slab)
    rows, block = rho_in.shape[0], planes * LANES
    spec = pl.BlockSpec((block, LANES), lambda s, m: (s, 0))
    const = lambda shape: pl.BlockSpec(shape, lambda s, m: (0,) * len(shape))
    return pl.pallas_call(
        middle_kernel,
        grid_spec=pltpu.PrefetchScalarGridSpec(
            num_scalar_prefetch=1,
            grid=(rows // block,),
            in_specs=[const(v.shape) for v in rho] + [spec, spec],
            out_specs=[spec, spec],
        ),
        out_shape=[jax.ShapeDtypeStruct((rows, LANES), f32), jax.ShapeDtypeStruct((rows, LANES), bf16)],
        compiler_params=pltpu.CompilerParams(vmem_limit_bytes=12 << 20),
        cost_estimate=pl.CostEstimate(flops=10**8, bytes_accessed=rows * LANES * 12, transcendentals=0),
        name="middle",
    )(me, *rho, rho_in, prev_mid)


def row_sum(v):
    return jnp.sum(v, axis=0, keepdims=True)


def dots_kernel(first, at_ref, *refs):
    q_count = DEPTH - 1
    mine_ref, got_ref, own_in, far_in, prev_ref, hist_ref = refs[:6]
    recent, (upper_ref, lower_ref, stats_ref, newest_ref, res_ref) = refs[6:-5], refs[-5:]
    summed = []
    for i in range(4):
        v = (mine_ref[i].astype(f32) + got_ref[i ^ 1].astype(f32)).astype(bf16)
        (upper_ref, lower_ref)[i // 2][i % 2] = v
        summed.append(v.astype(f32))
    half = mine_ref.shape[1]
    total = None
    for side, in_ref in enumerate((own_in, far_in)):
        rows = []
        for part in range(2):
            here = slice(part * half, (part + 1) * half)
            q = [hist_ref[j, side, here, :] for j in range(len(recent), q_count)] + [r[side, here, :] for r in recent]
            res = summed[2 * part + side] - in_ref[here, :]
            newest = res - prev_ref[side, here, :]
            newest_ref[side, here, :] = newest
            res_ref[side, here, :] = res
            out = [row_sum(v * newest) for v in q] + [row_sum(newest * newest)]
            out += [row_sum(v * res) for v in q] + [row_sum(newest * res)]
            if first:
                for j, k in pair_index(q_count):
                    out.append(row_sum(q[j] * q[k]))
            out += [jnp.zeros((1, LANES), f32)] * (STAT_ROWS - len(out))
            rows.append(jnp.concatenate(out, axis=0))
        table = rows[0] + rows[1]
        total = table if total is None else total + table
    table = jnp.sum(total, axis=1, keepdims=True)
    shape = (STAT_ROWS, LANES)
    lane = lax.broadcasted_iota(jnp.int32, shape, 1)
    own = lax.broadcasted_iota(jnp.int32, shape, 0)
    stats_ref[...] = row_sum(jnp.where(lane == own, jnp.broadcast_to(table, shape), 0.0))


def dots(first, at, mine, got, rho_in, prev_res, hist, recent):
    half = mine.shape[1]
    block = 2 * half
    const = lambda shape: pl.BlockSpec(shape, lambda s, m: (0,) * len(shape))
    pair = (2, block, LANES)
    return pl.pallas_call(
        functools.partial(dots_kernel, first),
        grid_spec=pltpu.PrefetchScalarGridSpec(
            num_scalar_prefetch=1,
            grid=(1,),
            in_specs=[
                const(mine.shape),
                const(got.shape),
                pl.BlockSpec((block, LANES), lambda s, m: (m[0], 0)),
                pl.BlockSpec((block, LANES), lambda s, m: (m[1], 0)),
                const(pair),
                const(hist.shape),
            ]
            + [const(pair)] * len(recent),
            out_specs=[const((2, half, LANES))] * 2 + [const((1, LANES)), const(pair), const(pair)],
        ),
        out_shape=[jax.ShapeDtypeStruct((2, half, LANES), bf16)] * 2
        + [
            jax.ShapeDtypeStruct((1, LANES), f32),
            jax.ShapeDtypeStruct(pair, f32),
            jax.ShapeDtypeStruct(pair, f32),
        ],
        compiler_params=pltpu.CompilerParams(vmem_limit_bytes=14 << 20),
        cost_estimate=pl.CostEstimate(flops=10**7, bytes_accessed=block * LANES * 64, transcendentals=0),
        name="dots",
    )(at, mine, got, rho_in, rho_in, prev_res, hist, *recent)


def mix_plane(me, coeffs, step, step_rows, base, rows, rho_refs, in_ref, prev_mid_ref, s_refs):
    rho_out = read_rows(rho_refs, step, step_rows, base, rows, me)
    here = pl.ds(base, rows)
    rho_in = in_ref[here, :]
    mid = mixing_weight * (rho_out + rho_in)
    dens = mid - coeffs[-1] * (mid - prev_mid_ref[here, :])
    for c, ref in zip(coeffs, s_refs):
        dens = dens - c * ref[here, :].astype(f32)
    return dens, rho_out - rho_in


def forward_kernel(kind, planes, first, groups, cells, me_ref, *refs):
    refs = list(refs)
    take = lambda k: [refs.pop(0) for _ in range(k)]
    mixing = kind != "plain"
    me = me_ref[0]
    if mixing:
        (stats_ref,) = take(1)
        carry_ref = None if first else take(1)[0]
        rho_refs = take(4)
        in_ref, prev_mid_ref = take(2)
        s_refs = take(DEPTH - 1)
    else:
        (in_ref,) = take(1)
    if kind != "last":
        ext_ref, psi_ref, wz_ref, ly_ref = take(4)
        out_refs = take(groups)
    if mixing:
        dens_ref, second = take(2)
        (coeff_ref,) = take(1)

        @pl.when(pl.program_id(0) == 0)
        def _():
            gram, rhs = finish_stats(stats_ref, carry_ref, first, cells)
            for j, c in enumerate(solve_rows(gram, rhs)):
                coeff_ref[j : j + 1, :] = c
            if kind == "mix":
                second[...] = jnp.zeros_like(second)
                for (j, k), i in pair_index(DEPTH - 1).items():
                    second[i : i + 1, :] = gram[j + 1][k + 1]

        coeffs = [coeff_ref[j : j + 1, :] for j in range(DEPTH)]
    if kind != "last":
        w_ref, a_ref, scratch = take(3)
    for xi in range(planes):
        here = pl.ds(xi * LANES, LANES)
        if mixing:
            dens, res = mix_plane(
                me, coeffs, pl.program_id(0), planes * LANES, xi * LANES, LANES,
                rho_refs, in_ref, prev_mid_ref, s_refs,
            )
            dens_ref[here, :] = dens
            if kind == "last":
                second[here, :] = res
        else:
            dens = in_ref[here, :]
        if kind != "last":
            factor = jnp.exp(-time_step * (ext_ref[here, :] + dens - energy_shift))
            for c in range(2):
                w_ref[here, c * LANES : (c + 1) * LANES] = (psi_ref[c, xi].astype(f32) * factor).astype(bf16)
    if kind == "last":
        return
    kept = ly_ref.shape[0] // 2
    sign = half_sign((kept, LANES), 1.0)
    a_ref[...] = dot(w_ref[...], wz_ref[...]).astype(bf16)
    for pair in pairs(planes):
        wide = [a_ref[xi * LANES : (xi + 1) * LANES, :] for xi in pair]
        t = dot(ly_ref[...], jnp.concatenate(wide, axis=1))
        for i, xi in enumerate(pair):
            lanes = slice(i * LANES, (i + 1) * LANES)
            out = t[:kept, lanes] + sign * swap_halves(t[kept:, lanes])
            scratch[pl.ds(xi, kept, stride=planes), :] = out
    per = kept // groups
    for g in range(groups):
        rows = scratch[g * per * planes : (g + 1) * per * planes, :]
        out_refs[g][...] = rows.reshape(per, planes, LANES).astype(bf16)


def table_spec(table):
    return pl.BlockSpec((None,) + table.shape[1:], lambda s, m: (m[1], 0, 0))


def pairs(count):
    return [tuple(range(i, min(i + 2, count))) for i in range(0, count, 2)]


def forward(kind, me, slab, groups, cells, ext=None, psi=None, band=0, wz=None, ly=None, density=None, mix=None):
    planes = min(PLANES, slab)
    steps = slab // planes
    block = planes * LANES
    rows = slab * LANES
    const = lambda shape: pl.BlockSpec(shape, lambda s, m: (0,) * len(shape))
    rowspec = pl.BlockSpec((block, LANES), lambda s, m: (s, 0))
    args, specs, outs, out_specs, scratch = [], [], [], [], []
    first = False
    if kind != "plain":
        first = mix["carry"] is None
        small = [mix["stats"]] + ([] if first else [mix["carry"]]) + list(mix["rho"])
        args += small
        specs += [const(v.shape) for v in small]
        wide = [mix["rho_in"], mix["prev_mid"]] + list(mix["orig"]) + list(mix["extra"])
        args += wide
        specs += [rowspec] * len(wide)
    else:
        args.append(density)
        specs.append(rowspec)
    if kind != "last":
        kept = ly.shape[1] // 2
        per = kept // groups
        args += [ext, psi, wz, ly]
        specs += [
            rowspec,
            pl.BlockSpec((2, None, planes, LANES, LANES), lambda s, m: (0, band, s, 0, 0)),
            const(wz.shape),
            table_spec(ly),
        ]
        outs += [jax.ShapeDtypeStruct((per, slab, LANES), bf16)] * groups
        out_specs += [pl.BlockSpec((per, planes, LANES), lambda s, m: (0, s, 0))] * groups
    if kind != "plain":
        outs.append(jax.ShapeDtypeStruct((rows, LANES), f32))
        out_specs.append(rowspec)
        if kind == "mix":
            outs.append(jax.ShapeDtypeStruct((CARRY_ROWS, LANES), f32))
            out_specs.append(const((CARRY_ROWS, LANES)))
        else:
            outs.append(jax.ShapeDtypeStruct((rows, LANES), f32))
            out_specs.append(rowspec)
        scratch.append(pltpu.VMEM((8, LANES), f32))
    if kind != "last":
        scratch += [
            pltpu.VMEM((block, 2 * LANES), bf16),
            pltpu.VMEM((block, LANES), bf16),
            pltpu.VMEM((kept * planes, LANES), f32),
        ]
    return pl.pallas_call(
        functools.partial(forward_kernel, kind, planes, first, groups, cells),
        grid_spec=pltpu.PrefetchScalarGridSpec(
            num_scalar_prefetch=1, grid=(steps,), in_specs=specs, out_specs=out_specs, scratch_shapes=scratch
        ),
        out_shape=outs,
        compiler_params=pltpu.CompilerParams(vmem_limit_bytes=20 << 20),
        cost_estimate=pl.CostEstimate(flops=10**9, bytes_accessed=6 << 20, transcendentals=0),
        name="forward_" + kind,
    )(me, *args)


def filter_kernel(groups, me_ref, *refs):
    in_refs, refs = refs[:groups], refs[groups:]
    lf_ref, li_ref, kin_ref = refs[:3]
    out_refs = refs[3:]
    per, slab, _ = in_refs[0].shape
    kept = lf_ref.shape[0] // 2
    fsign = half_sign((kept, LANES), 1.0)
    isign = half_sign((kept, LANES), -1.0)
    for pair in pairs(per):
        wide = [jnp.concatenate([r[k] for r in in_refs], axis=0) for k in pair]
        t = dot(lf_ref[...], jnp.concatenate(wide, axis=1))
        both = []
        for i, k in enumerate(pair):
            lanes = slice(i * LANES, (i + 1) * LANES)
            c = (t[:kept, lanes] + fsign * swap_halves(t[kept:, lanes])) * kin_ref[k]
            both.append(jnp.concatenate([c.astype(bf16), (isign * swap_halves(c)).astype(bf16)], axis=0))
        d = dot(li_ref[...], jnp.concatenate(both, axis=1)).astype(bf16)
        for i, k in enumerate(pair):
            for g in range(groups):
                out_refs[g][k] = d[g * slab : (g + 1) * slab, i * LANES : (i + 1) * LANES]


def x_filter(me, blocks, lf, li, kinetic):
    groups = len(blocks)
    per, slab, _ = blocks[0].shape
    split = FILTER_STEPS if per % (2 * FILTER_STEPS) == 0 else 1
    spec = pl.BlockSpec((per // split, slab, LANES), lambda s, m: (s, 0, 0))
    return pl.pallas_call(
        functools.partial(filter_kernel, groups),
        grid_spec=pltpu.PrefetchScalarGridSpec(
            num_scalar_prefetch=1,
            grid=(split,),
            in_specs=[spec] * groups
            + [
                table_spec(lf),
                table_spec(li),
                pl.BlockSpec((per // split,) + kinetic.shape[1:], lambda s, m: (s, 0, 0)),
            ],
            out_specs=[spec] * groups,
        ),
        out_shape=[jax.ShapeDtypeStruct(blocks[0].shape, bf16)] * groups,
        compiler_params=pltpu.CompilerParams(vmem_limit_bytes=12 << 20),
        cost_estimate=pl.CostEstimate(flops=5 * 10**8, bytes_accessed=2 << 20, transcendentals=0),
        name="x_filter",
    )(me, *blocks, lf, li, kinetic)


def inverse_kernel(groups, planes, scale, band, adds, ends, keep_psi, me_ref, *refs):
    in_refs, refs = refs[:groups], refs[groups:]
    occ_ref, liy_ref, wiz_ref = refs[:3]
    refs = list(refs[3:])
    if adds:
        part_ref = refs.pop(0)
    if keep_psi:
        psi_ref = refs.pop(0)
    if ends:
        rho_refs = [refs.pop(0) for _ in range(2)]
    else:
        total_ref = refs.pop(0)
    scratch, e_ref = refs
    me = me_ref[0]
    per = in_refs[0].shape[0]
    kept = per * groups
    isign = half_sign((kept, LANES), -1.0)
    for g in range(groups):
        scratch[g * per * planes : (g + 1) * per * planes, :] = (
            in_refs[g][...].astype(f32).reshape(per * planes, LANES)
        )
    for pair in pairs(planes):
        both = []
        for xi in pair:
            v = scratch[pl.ds(xi, kept, stride=planes), :]
            both.append(jnp.concatenate([v.astype(bf16), (isign * swap_halves(v)).astype(bf16)], axis=0))
        e = dot(liy_ref[...], jnp.concatenate(both, axis=1)).astype(bf16)
        for i, xi in enumerate(pair):
            e_ref[xi * LANES : (xi + 1) * LANES, :] = e[:, i * LANES : (i + 1) * LANES]
    for xi in range(planes):
        here = pl.ds(xi * LANES, LANES)
        psi = dot(e_ref[here, :], wiz_ref[...]).astype(bf16)
        re, im = psi[:, :LANES], psi[:, LANES:]
        if keep_psi:
            psi_ref[0, xi] = re
            psi_ref[1, xi] = im
        re, im = re.astype(f32), im.astype(f32)
        total = (occ_ref[band] * scale) * (re * re + im * im)
        if adds:
            total = total + part_ref[here, :]
        if ends:
            write_rows(rho_refs, pl.program_id(0), planes * LANES, xi * LANES, total.astype(bf16), me)
        else:
            total_ref[here, :] = total


def inverse(me, blocks, occ, band, bands, liy, wiz, band_devices, scale, keep_psi, part):
    groups = len(blocks)
    per, slab, _ = blocks[0].shape
    planes = min(PLANES, slab)
    rows, block = slab * LANES, planes * LANES
    half = rows // band_devices // 2
    adds, ends = part is not None, band == bands - 1
    spec = pl.BlockSpec((per, planes, LANES), lambda s, m: (0, s, 0))
    rowspec = pl.BlockSpec((block, LANES), lambda s, m: (s, 0))
    const = lambda shape: pl.BlockSpec(shape, lambda s, m: (0,) * len(shape))
    outs, out_specs = [], []
    if keep_psi:
        outs.append(jax.ShapeDtypeStruct((2, 1, slab, LANES, LANES), bf16))
        out_specs.append(pl.BlockSpec((2, None, planes, LANES, LANES), lambda s, m: (0, 0, s, 0, 0)))
    if ends:
        outs += [jax.ShapeDtypeStruct((band_devices, half, LANES), bf16)] * 2
        out_specs += [const(outs[-1].shape)] * 2
    else:
        outs.append(jax.ShapeDtypeStruct((rows, LANES), f32))
        out_specs.append(rowspec)
    return pl.pallas_call(
        functools.partial(inverse_kernel, groups, planes, scale, band, adds, ends, keep_psi),
        grid_spec=pltpu.PrefetchScalarGridSpec(
            num_scalar_prefetch=1,
            grid=(slab // planes,),
            in_specs=[spec] * groups
            + [pl.BlockSpec(memory_space=pltpu.SMEM), table_spec(liy), const(wiz.shape)]
            + ([rowspec] if adds else []),
            out_specs=out_specs,
            scratch_shapes=[
                pltpu.VMEM((per * groups * planes, LANES), f32),
                pltpu.VMEM((block, LANES), bf16),
            ],
        ),
        out_shape=outs,
        compiler_params=pltpu.CompilerParams(vmem_limit_bytes=16 << 20),
        cost_estimate=pl.CostEstimate(flops=10**9, bytes_accessed=4 << 20, transcendentals=0),
        name="inverse",
    )(me, *blocks, occ, liy, wiz, *([part] if adds else []))


def partner(v, axis, size, mask):
    return lax.ppermute(v, axis, [(i, i ^ mask) for i in range(size)])


def exchange(blocks, axis, size):
    if size > 4:
        index = lax.axis_index(axis)
        order = jnp.arange(size, dtype=jnp.int32) ^ index
        stacked = jnp.stack(blocks)[order]
        got = lax.all_to_all(stacked, axis, 0, 0)[order]
        return [got[m] for m in range(size)]
    return [blocks[0]] + [partner(blocks[m], axis, size, m) for m in range(1, size)]


def add_pair(mine, got):
    return (mine.astype(f32) + got.astype(f32)).astype(bf16)


def reduce_blocks(upper, lower, axis, size, fill):
    both = [upper, lower]
    steps = list(zip(*orders(size)))
    for bits in steps[:-1]:
        cut = both[0].shape[0] // 2
        got = [partner(v[cut:], axis, size, 1 << bit) for v, bit in zip(both, bits)]
        if fill is not None:
            got, fill = lax.optimization_barrier((got, fill))
            filled, fill = fill, None
        both = [add_pair(v[:cut], g) for v, g in zip(both, got)]
    mine = jnp.concatenate(both, axis=0)
    return mine, partner(mine, axis, size, 1 << steps[-1][0]), filled


def gather_blocks(both, stats, axis, size, grid, grid_size):
    steps = list(reversed(list(zip(*orders(size)))[:-1]))
    stats = sum_direct(stats, grid, range(grid_size), grid_size)
    for i, bits in enumerate(steps):
        if i:
            both = [jnp.concatenate(v, axis=0) for v in both]
            both, stats = lax.optimization_barrier((both, stats))
        both = [[v, partner(v, axis, size, 1 << bit)] for v, bit in zip(both, bits)]
    return both[0] + both[1], sum_direct(stats, axis, range(size // 2), size)


def sum_direct(v, axis, masks, size):
    if size > 8:
        for bit in range(len(masks).bit_length() - 1):
            v = v + partner(v, axis, size, 1 << bit)
        return v
    terms = [v] + [partner(v, axis, size, m) for m in masks if m]
    while len(terms) > 1:
        terms = [terms[i] + terms[i + 1] for i in range(0, len(terms), 2)]
    return terms[0]


def local(
    bands,
    occupations,
    external,
    density_in,
    prev_density,
    prev_residual,
    hist_density,
    hist_residual,
):
    groups = lax.axis_size("grid")
    band_devices = lax.axis_size("band")
    slab, ng = external.shape[:2]
    nbands = bands.shape[1]
    cells = float(ng) ** 3
    scale = density_scale / (occupations.shape[0] * band_devices)
    rows = slab * ng
    kept = ng // 2
    per = kept // groups
    wz, wiz, ly, liy, lf, li = fourier_tables(ng, groups)
    grid_at = lax.axis_index("grid").astype(jnp.int32)
    shape = (per, kept, 2 * kept)
    squared = lambda v: ((v - kept // 2) * (v - kept // 2)).astype(f32)
    place = lambda d: lax.broadcasted_iota(jnp.int32, shape, d)
    radius = squared(place(0) + grid_at * per) + squared(place(1)) + squared(place(2) % kept)
    quarter = ng / 4.0
    kinetic = jnp.exp(-time_step * radius / (quarter * quarter))
    band_at = lax.axis_index("band").astype(jnp.int32)
    me = jnp.stack([band_at, grid_at])

    flat = lambda v: v.reshape(v.shape[:-3] + (rows, ng))
    ext, rho_in, prev_in, prev_res = map(flat, (external, density_in, prev_density, prev_residual))
    hist_r, hist_q = flat(hist_density), flat(hist_residual)
    psi = [(bands, b) for b in range(nbands)]
    block = rows // band_devices
    ends = jnp.stack([band_at, band_at ^ (band_devices // 2)])
    two = lambda v, axis, at: jnp.stack(
        [lax.dynamic_slice_in_dim(v, at[i] * block, block, axis) for i in range(2)], axis=axis
    )
    hist_pair, prev_res_pair = two(hist_q, 1, ends), two(prev_res, 0, ends)
    parts = max(1, slab // 8)
    extra = []
    new_q = []
    carry = None
    mix = None
    common = dict(ext=ext, wz=wz, ly=ly)
    for iteration in range(ITERS):
        blocks = []
        for b, (array, at) in enumerate(psi):
            if iteration and b == 0:
                out = forward("mix", me, slab, groups, cells, psi=array, band=at, mix=mix, **common)
                rho_in, carry = out[groups:]
            else:
                out = forward("plain", me, slab, groups, cells, psi=array, band=at, density=rho_in, **common)
            blocks.append(exchange(out[:groups], "grid", groups))
        for b in range(nbands):
            blocks[b] = exchange(x_filter(me, blocks[b], lf, li, kinetic), "grid", groups)
        last = iteration == ITERS - 1
        part = None
        psi = []
        for b in range(nbands):
            out = inverse(
                me, blocks[b], occupations, b, nbands, liy, wiz, band_devices, scale, not last, part
            )
            if not last:
                psi.append((out[0], 0))
                out = out[1:]
            part = out[0]
        out = list(out)
        if iteration == 0:
            out[0], tie, late_in = lax.optimization_barrier((out[0], ends, prev_in))
            fill = (
                [combine(tie, hist_r, hist_q, j, parts) for j in range(DEPTH - 1)],
                late_in + mixing_weight * prev_res,
            )
        else:
            out[0], rho, prev_mid = lax.optimization_barrier((out[0], mix["rho"], mix["prev_mid"]))
            prev_mid, newest_s = middle(me, slab, rho, mix["rho_in"], prev_mid)
            fill = (orig[1:], prev_mid, extra + [newest_s])
        mine, got, fill = reduce_blocks(out[0], out[1], "band", band_devices, fill)
        orig, prev_mid = fill[:2]
        if iteration:
            extra = fill[2]
        upper, lower, stats, newest_q, prev_res_pair = dots(
            iteration == 0, ends, mine, got, rho_in, prev_res_pair, hist_pair, new_q
        )
        new_q = new_q + [newest_q]
        rho, stats = gather_blocks([upper, lower], stats, "band", band_devices, "grid", groups)
        mix = dict(stats=stats, carry=carry, rho=rho, rho_in=rho_in,
                   prev_mid=prev_mid, orig=orig, extra=extra)
    density, residual = forward("last", me, slab, groups, cells, mix=mix)
    unflat = lambda v: v.reshape(slab, ng, ng)
    return unflat(density), unflat(residual)


def solution(mesh):
    placed = (
        P(None, "band", "grid", None, None),
        P("band"),
        P("grid", None, None),
        P("grid", None, None),
        P("grid", None, None),
        P("grid", None, None),
        P(None, "grid", None, None),
        P(None, "grid", None, None),
    )
    return jax.shard_map(
        local,
        mesh=mesh,
        in_specs=placed,
        out_specs=(P("grid", None, None), P("grid", None, None)),
        check_vma=False,
    )
```

```python
import functools
import math

import jax
import jax.numpy as jnp
import ml_dtypes
import numpy as np
from jax import lax
from jax.experimental import pallas as pl
from jax.experimental.pallas import tpu as pltpu
from jax.sharding import PartitionSpec as P


DEPTH = 6
ITERS = 3
LANES = 128
PLANES = 16
FILTER_STEPS = 1

time_step = 0.25
energy_shift = 2.5
mixing_weight = 0.5
ridge_share = 0.1
ridge_floor = 0.01
density_scale = 8.0


f32 = jnp.float32
bf16 = jnp.bfloat16


def fourier_tables(length, groups):
    frequency = np.arange(-(length // 4), length // 4)
    phase_index = np.arange(length)[:, None] * frequency[None, :] % length
    angles = phase_index.astype(np.float32) * np.float32(2.0 * math.pi / length)
    unit_scale = np.float32(1.0 / math.sqrt(length))
    cos, sin = (f(angles).astype(np.float32) * unit_scale for f in (np.cos, np.sin))
    out = [
        np.block([[cos, -sin], [sin, cos]]),
        np.block([[cos.T, sin.T], [-sin.T, cos.T]]),
    ]
    stacks = [[], [], [], []]
    for index in range(groups):
        def ordered(count):
            return np.concatenate([np.arange(count // groups) + (index ^ m) * (count // groups) for m in range(groups)])

        ck, sk = (v[:, ordered(len(frequency))] for v in (cos, sin))
        cx, sx = (v[ordered(length)] for v in (cos, sin))
        stacks[0].append(np.concatenate([ck.T, sk.T], axis=0))
        stacks[1].append(np.concatenate([ck, sk], axis=1))
        stacks[2].append(np.concatenate([cx.T, sx.T], axis=0))
        stacks[3].append(np.concatenate([cx, sx], axis=1))
    return [jnp.asarray(v.astype(ml_dtypes.bfloat16)) for v in out + [np.stack(v) for v in stacks]]


def dot(a, b):
    return jnp.dot(a, b, preferred_element_type=f32)


def swap_halves(v):
    return pltpu.roll(v, v.shape[-1] // 2, v.ndim - 1)


def half_sign(shape, first):
    lane = lax.broadcasted_iota(jnp.int32, shape, len(shape) - 1)
    return jnp.where(lane < shape[-1] // 2, first, -first).astype(f32)


def orders(devices):
    bits = devices.bit_length() - 1
    upper = list(range(bits))
    lower = ([1, 0] + upper[2:]) if bits > 1 else upper
    return upper, lower


def position(relative, order):
    out = None
    for i, bit in enumerate(order):
        part = lax.shift_left(lax.bitwise_and(lax.shift_right_logical(relative, bit), 1), len(order) - 1 - i)
        out = part if out is None else out + part
    return out


def units(half, devices, step, step_rows, row, count, me):
    assert step_rows % (2 * half) == 0
    unit = min(count, half)
    for at in range(0, count, unit):
        block, within = divmod(row + at, 2 * half)
        which, offset = divmod(within, half)
        relative = lax.bitwise_xor(step * (step_rows // (2 * half)) + block, me)
        yield which, position(relative, orders(devices)[which]), offset, at, unit


def read_rows(refs, step, step_rows, row, count, me):
    near, half = refs[0].shape[:2]
    out = []
    for which, at, offset, _, unit in units(half, 2 * near, step, step_rows, row, count, me):
        here = (lax.rem(at, near), pl.ds(offset, unit), slice(None))
        low, high = (refs[2 * which + i][here].astype(f32) for i in range(2))
        out.append(jnp.where(at < near, low, high))
    return out[0] if len(out) == 1 else jnp.concatenate(out, axis=0)


def write_rows(refs, step, step_rows, row, value, me):
    devices, half = refs[0].shape[:2]
    for which, to, offset, at, unit in units(half, devices, step, step_rows, row, value.shape[0], me):
        refs[which][to, pl.ds(offset, unit), :] = value[at : at + unit]


def solve_rows(gram, rhs):
    n = len(rhs)
    trace = gram[0][0]
    for j in range(1, n):
        trace = trace + gram[j][j]
    ridge = ridge_share * trace / n + ridge_floor
    a = [[gram[j][k] + ridge if j == k else gram[j][k] for k in range(n)] for j in range(n)]
    low = [[None] * n for _ in range(n)]
    diag = [None] * n
    inv = [None] * n
    for j in range(n):
        value = a[j][j]
        scaled = []
        for k in range(j):
            s = low[j][k] * diag[k]
            scaled.append(s)
            value = value - low[j][k] * s
        diag[j] = value
        inv[j] = 1.0 / value
        for r in range(j + 1, n):
            e = a[r][j]
            for k in range(j):
                e = e - low[r][k] * scaled[k]
            low[r][j] = e * inv[j]
    mid = []
    for j in range(n):
        e = rhs[j]
        for k in range(j):
            e = e - low[j][k] * mid[k]
        mid.append(e)
    out = [None] * n
    for j in reversed(range(n)):
        e = mid[j] * inv[j]
        for k in range(j + 1, n):
            e = e - low[k][j] * out[k]
        out[j] = e
    return out


def pair_index(n):
    return {(j, k): i for i, (j, k) in enumerate((j, k) for j in range(n) for k in range(j, n))}


STAT_ROWS = 32


def spread_diagonal(row):
    shape = (STAT_ROWS, LANES)
    lane = lax.broadcasted_iota(jnp.int32, shape, 1)
    own = lax.broadcasted_iota(jnp.int32, shape, 0)
    picked = jnp.where(lane == own, jnp.broadcast_to(row, shape), 0.0)
    return jnp.broadcast_to(jnp.sum(picked, axis=1, keepdims=True), shape)


def finish_stats(stats_ref, carry_ref, first, cells):
    total = spread_diagonal(stats_ref[...] * (1.0 / cells))
    n = DEPTH
    gram = [[None] * n for _ in range(n)]
    kept = pair_index(n - 1)
    for (j, k), i in kept.items():
        value = total[2 * n + i : 2 * n + i + 1] if first else carry_ref[i : i + 1, :]
        gram[j][k] = value
        gram[k][j] = value
    for j in range(n):
        value = total[j : j + 1]
        gram[j][n - 1] = value
        gram[n - 1][j] = value
    rhs = [total[n + j : n + j + 1] for j in range(n)]
    return gram, rhs


CARRY_ROWS = 16


def combine_kernel(tie_ref, r_ref, q_ref, s_ref):
    s_ref[...] = (r_ref[...] + mixing_weight * q_ref[...]).astype(s_ref.dtype)


def combine(tie, hist_density, hist_residual, j, parts):
    _, rows, lanes = hist_density.shape
    block = rows // parts
    spec = pl.BlockSpec((None, block, lanes), lambda s, t: (j, s, 0))
    return pl.pallas_call(
        combine_kernel,
        grid_spec=pltpu.PrefetchScalarGridSpec(
            num_scalar_prefetch=1,
            grid=(parts,),
            in_specs=[spec, spec],
            out_specs=pl.BlockSpec((block, lanes), lambda s, t: (s, 0)),
        ),
        out_shape=jax.ShapeDtypeStruct((rows, lanes), bf16),
        compiler_params=pltpu.CompilerParams(vmem_limit_bytes=12 << 20),
        cost_estimate=pl.CostEstimate(flops=10**8, bytes_accessed=rows * lanes * 10, transcendentals=0),
        name="combine",
    )(tie, hist_density, hist_residual)


def middle_kernel(me_ref, *refs):
    rho_refs, (in_ref, prev_ref, mid_ref, new_ref) = refs[:4], refs[4:]
    rows = in_ref.shape[0]
    for base in range(0, rows, LANES):
        here = pl.ds(base, LANES)
        rho_out = read_rows(rho_refs, pl.program_id(0), rows, base, LANES, me_ref[0])
        mid = mixing_weight * (rho_out + in_ref[here, :])
        mid_ref[here, :] = mid
        new_ref[here, :] = (mid - prev_ref[here, :]).astype(new_ref.dtype)


def middle(me, slab, rho, rho_in, prev_mid):
    planes = min(PLANES, slab)
    rows, block = rho_in.shape[0], planes * LANES
    spec = pl.BlockSpec((block, LANES), lambda s, m: (s, 0))
    const = lambda shape: pl.BlockSpec(shape, lambda s, m: (0,) * len(shape))
    return pl.pallas_call(
        middle_kernel,
        grid_spec=pltpu.PrefetchScalarGridSpec(
            num_scalar_prefetch=1,
            grid=(rows // block,),
            in_specs=[const(v.shape) for v in rho] + [spec, spec],
            out_specs=[spec, spec],
        ),
        out_shape=[jax.ShapeDtypeStruct((rows, LANES), f32), jax.ShapeDtypeStruct((rows, LANES), bf16)],
        compiler_params=pltpu.CompilerParams(vmem_limit_bytes=12 << 20),
        cost_estimate=pl.CostEstimate(flops=10**8, bytes_accessed=rows * LANES * 12, transcendentals=0),
        name="middle",
    )(me, *rho, rho_in, prev_mid)


def row_sum(v):
    return jnp.sum(v, axis=0, keepdims=True)


def finish_kernel(mine_ref, got_ref, upper_ref, lower_ref):
    for i in range(4):
        v = (mine_ref[i].astype(f32) + got_ref[i ^ 1].astype(f32)).astype(bf16)
        (upper_ref, lower_ref)[i // 2][i % 2] = v


def finish(mine, got):
    return pl.pallas_call(
        finish_kernel,
        out_shape=[jax.ShapeDtypeStruct((2,) + mine.shape[1:], bf16)] * 2,
        compiler_params=pltpu.CompilerParams(vmem_limit_bytes=8 << 20),
        cost_estimate=pl.CostEstimate(flops=10**6, bytes_accessed=3 * mine.size, transcendentals=0),
        name="finish",
    )(mine, got)


def dots_kernel(first, at_ref, *refs):
    q_count = DEPTH - 1
    upper_ref, lower_ref, own_in, far_in, prev_ref, hist_ref = refs[:6]
    recent, (stats_ref, newest_ref, res_ref) = refs[6:-3], refs[-3:]
    half = upper_ref.shape[1]
    total = None
    for side, in_ref in enumerate((own_in, far_in)):
        rows = []
        for part in range(2):
            here = slice(part * half, (part + 1) * half)
            q = [hist_ref[j, side, here, :] for j in range(len(recent), q_count)] + [r[side, here, :] for r in recent]
            res = (upper_ref, lower_ref)[part][side].astype(f32) - in_ref[here, :]
            newest = res - prev_ref[side, here, :]
            newest_ref[side, here, :] = newest
            res_ref[side, here, :] = res
            out = [row_sum(v * newest) for v in q] + [row_sum(newest * newest)]
            out += [row_sum(v * res) for v in q] + [row_sum(newest * res)]
            if first:
                for j, k in pair_index(q_count):
                    out.append(row_sum(q[j] * q[k]))
            out += [jnp.zeros((1, LANES), f32)] * (STAT_ROWS - len(out))
            rows.append(jnp.concatenate(out, axis=0))
        table = rows[0] + rows[1]
        total = table if total is None else total + table
    table = jnp.sum(total, axis=1, keepdims=True)
    shape = (STAT_ROWS, LANES)
    lane = lax.broadcasted_iota(jnp.int32, shape, 1)
    own = lax.broadcasted_iota(jnp.int32, shape, 0)
    stats_ref[...] = row_sum(jnp.where(lane == own, jnp.broadcast_to(table, shape), 0.0))


def dots(first, at, upper, lower, rho_in, prev_res, hist, recent):
    half = upper.shape[1]
    block = 2 * half
    const = lambda shape: pl.BlockSpec(shape, lambda s, m: (0,) * len(shape))
    pair = (2, block, LANES)
    return pl.pallas_call(
        functools.partial(dots_kernel, first),
        grid_spec=pltpu.PrefetchScalarGridSpec(
            num_scalar_prefetch=1,
            grid=(1,),
            in_specs=[
                const(upper.shape),
                const(lower.shape),
                pl.BlockSpec((block, LANES), lambda s, m: (m[0], 0)),
                pl.BlockSpec((block, LANES), lambda s, m: (m[1], 0)),
                const(pair),
                const(hist.shape),
            ]
            + [const(pair)] * len(recent),
            out_specs=[const((1, LANES)), const(pair), const(pair)],
        ),
        out_shape=[
            jax.ShapeDtypeStruct((1, LANES), f32),
            jax.ShapeDtypeStruct(pair, f32),
            jax.ShapeDtypeStruct(pair, f32),
        ],
        compiler_params=pltpu.CompilerParams(vmem_limit_bytes=14 << 20),
        cost_estimate=pl.CostEstimate(flops=1, bytes_accessed=block * LANES * 64, transcendentals=0),
        name="dots",
    )(at, upper, lower, rho_in, rho_in, prev_res, hist, *recent)


def mix_plane(me, coeffs, step, step_rows, base, rows, rho_refs, in_ref, prev_mid_ref, s_refs):
    rho_out = read_rows(rho_refs, step, step_rows, base, rows, me)
    here = pl.ds(base, rows)
    rho_in = in_ref[here, :]
    mid = mixing_weight * (rho_out + rho_in)
    dens = mid - coeffs[-1] * (mid - prev_mid_ref[here, :])
    for c, ref in zip(coeffs, s_refs):
        dens = dens - c * ref[here, :].astype(f32)
    return dens, rho_out - rho_in


def forward_kernel(kind, planes, first, groups, cells, me_ref, *refs):
    refs = list(refs)
    take = lambda k: [refs.pop(0) for _ in range(k)]
    mixing = kind != "plain"
    me = me_ref[0]
    if mixing:
        (stats_ref,) = take(1)
        carry_ref = None if first else take(1)[0]
        rho_refs = take(4)
        in_ref, prev_mid_ref = take(2)
        s_refs = take(DEPTH - 1)
    else:
        (in_ref,) = take(1)
    if kind != "last":
        ext_ref, psi_ref, wz_ref, ly_ref = take(4)
        out_refs = take(groups)
    if mixing:
        dens_ref, second = take(2)
        (coeff_ref,) = take(1)

        @pl.when(pl.program_id(0) == 0)
        def _():
            gram, rhs = finish_stats(stats_ref, carry_ref, first, cells)
            for j, c in enumerate(solve_rows(gram, rhs)):
                coeff_ref[j : j + 1, :] = c
            if kind == "mix":
                second[...] = jnp.zeros_like(second)
                for (j, k), i in pair_index(DEPTH - 1).items():
                    second[i : i + 1, :] = gram[j + 1][k + 1]

        coeffs = [coeff_ref[j : j + 1, :] for j in range(DEPTH)]
    if kind != "last":
        w_ref, a_ref, scratch = take(3)
    for xi in range(planes):
        here = pl.ds(xi * LANES, LANES)
        if mixing:
            dens, res = mix_plane(
                me, coeffs, pl.program_id(0), planes * LANES, xi * LANES, LANES,
                rho_refs, in_ref, prev_mid_ref, s_refs,
            )
            dens_ref[here, :] = dens
            if kind == "last":
                second[here, :] = res
        else:
            dens = in_ref[here, :]
        if kind != "last":
            factor = jnp.exp(-time_step * (ext_ref[here, :] + dens - energy_shift))
            for c in range(2):
                w_ref[here, c * LANES : (c + 1) * LANES] = (psi_ref[c, xi].astype(f32) * factor).astype(bf16)
    if kind == "last":
        return
    kept = ly_ref.shape[0] // 2
    sign = half_sign((kept, LANES), 1.0)
    a_ref[...] = dot(w_ref[...], wz_ref[...]).astype(bf16)
    for pair in pairs(planes):
        wide = [a_ref[xi * LANES : (xi + 1) * LANES, :] for xi in pair]
        t = dot(ly_ref[...], jnp.concatenate(wide, axis=1))
        for i, xi in enumerate(pair):
            lanes = slice(i * LANES, (i + 1) * LANES)
            out = t[:kept, lanes] + sign * swap_halves(t[kept:, lanes])
            scratch[pl.ds(xi, kept, stride=planes), :] = out
    per = kept // groups
    for g in range(groups):
        rows = scratch[g * per * planes : (g + 1) * per * planes, :]
        out_refs[g][...] = rows.reshape(per, planes, LANES).astype(bf16)


def table_spec(table):
    return pl.BlockSpec((None,) + table.shape[1:], lambda s, m: (m[1], 0, 0))


def pairs(count):
    return [tuple(range(i, min(i + 2, count))) for i in range(0, count, 2)]


def forward(kind, me, slab, groups, cells, ext=None, psi=None, band=0, wz=None, ly=None, density=None, mix=None):
    planes = min(PLANES, slab)
    steps = slab // planes
    block = planes * LANES
    rows = slab * LANES
    const = lambda shape: pl.BlockSpec(shape, lambda s, m: (0,) * len(shape))
    rowspec = pl.BlockSpec((block, LANES), lambda s, m: (s, 0))
    args, specs, outs, out_specs, scratch = [], [], [], [], []
    first = False
    if kind != "plain":
        first = mix["carry"] is None
        small = [mix["stats"]] + ([] if first else [mix["carry"]]) + list(mix["rho"])
        args += small
        specs += [const(v.shape) for v in small]
        wide = [mix["rho_in"], mix["prev_mid"]] + list(mix["orig"]) + list(mix["extra"])
        args += wide
        specs += [rowspec] * len(wide)
    else:
        args.append(density)
        specs.append(rowspec)
    if kind != "last":
        kept = ly.shape[1] // 2
        per = kept // groups
        args += [ext, psi, wz, ly]
        specs += [
            rowspec,
            pl.BlockSpec((2, None, planes, LANES, LANES), lambda s, m: (0, band, s, 0, 0)),
            const(wz.shape),
            table_spec(ly),
        ]
        outs += [jax.ShapeDtypeStruct((per, slab, LANES), bf16)] * groups
        out_specs += [pl.BlockSpec((per, planes, LANES), lambda s, m: (0, s, 0))] * groups
    if kind != "plain":
        outs.append(jax.ShapeDtypeStruct((rows, LANES), f32))
        out_specs.append(rowspec)
        if kind == "mix":
            outs.append(jax.ShapeDtypeStruct((CARRY_ROWS, LANES), f32))
            out_specs.append(const((CARRY_ROWS, LANES)))
        else:
            outs.append(jax.ShapeDtypeStruct((rows, LANES), f32))
            out_specs.append(rowspec)
        scratch.append(pltpu.VMEM((8, LANES), f32))
    if kind != "last":
        scratch += [
            pltpu.VMEM((block, 2 * LANES), bf16),
            pltpu.VMEM((block, LANES), bf16),
            pltpu.VMEM((kept * planes, LANES), f32),
        ]
    return pl.pallas_call(
        functools.partial(forward_kernel, kind, planes, first, groups, cells),
        grid_spec=pltpu.PrefetchScalarGridSpec(
            num_scalar_prefetch=1, grid=(steps,), in_specs=specs, out_specs=out_specs, scratch_shapes=scratch
        ),
        out_shape=outs,
        compiler_params=pltpu.CompilerParams(vmem_limit_bytes=20 << 20),
        cost_estimate=pl.CostEstimate(flops=10**9, bytes_accessed=6 << 20, transcendentals=0),
    )(me, *args)


def filter_kernel(groups, me_ref, *refs):
    in_refs, refs = refs[:groups], refs[groups:]
    lf_ref, li_ref, kin_ref = refs[:3]
    out_refs = refs[3:]
    per, slab, _ = in_refs[0].shape
    kept = lf_ref.shape[0] // 2
    fsign = half_sign((kept, LANES), 1.0)
    isign = half_sign((kept, LANES), -1.0)
    for pair in pairs(per):
        wide = [jnp.concatenate([r[k] for r in in_refs], axis=0) for k in pair]
        t = dot(lf_ref[...], jnp.concatenate(wide, axis=1))
        both = []
        for i, k in enumerate(pair):
            lanes = slice(i * LANES, (i + 1) * LANES)
            c = (t[:kept, lanes] + fsign * swap_halves(t[kept:, lanes])) * kin_ref[k]
            both.append(jnp.concatenate([c.astype(bf16), (isign * swap_halves(c)).astype(bf16)], axis=0))
        d = dot(li_ref[...], jnp.concatenate(both, axis=1)).astype(bf16)
        for i, k in enumerate(pair):
            for g in range(groups):
                out_refs[g][k] = d[g * slab : (g + 1) * slab, i * LANES : (i + 1) * LANES]


def x_filter(me, blocks, lf, li, kinetic):
    groups = len(blocks)
    per, slab, _ = blocks[0].shape
    split = FILTER_STEPS if per % (2 * FILTER_STEPS) == 0 else 1
    spec = pl.BlockSpec((per // split, slab, LANES), lambda s, m: (s, 0, 0))
    return pl.pallas_call(
        functools.partial(filter_kernel, groups),
        grid_spec=pltpu.PrefetchScalarGridSpec(
            num_scalar_prefetch=1,
            grid=(split,),
            in_specs=[spec] * groups
            + [
                table_spec(lf),
                table_spec(li),
                pl.BlockSpec((per // split,) + kinetic.shape[1:], lambda s, m: (s, 0, 0)),
            ],
            out_specs=[spec] * groups,
        ),
        out_shape=[jax.ShapeDtypeStruct(blocks[0].shape, bf16)] * groups,
        compiler_params=pltpu.CompilerParams(vmem_limit_bytes=12 << 20),
        cost_estimate=pl.CostEstimate(flops=5 * 10**8, bytes_accessed=2 << 20, transcendentals=0),
        name="x_filter",
    )(me, *blocks, lf, li, kinetic)


def inverse_kernel(groups, planes, scale, band, adds, ends, keep_psi, me_ref, *refs):
    in_refs, refs = refs[:groups], refs[groups:]
    occ_ref, liy_ref, wiz_ref = refs[:3]
    refs = list(refs[3:])
    if adds:
        part_ref = refs.pop(0)
    if keep_psi:
        psi_ref = refs.pop(0)
    if ends:
        rho_refs = [refs.pop(0) for _ in range(2)]
    else:
        total_ref = refs.pop(0)
    scratch, e_ref = refs
    me = me_ref[0]
    per = in_refs[0].shape[0]
    kept = per * groups
    isign = half_sign((kept, LANES), -1.0)
    for g in range(groups):
        scratch[g * per * planes : (g + 1) * per * planes, :] = (
            in_refs[g][...].astype(f32).reshape(per * planes, LANES)
        )
    for pair in pairs(planes):
        both = []
        for xi in pair:
            v = scratch[pl.ds(xi, kept, stride=planes), :]
            both.append(jnp.concatenate([v.astype(bf16), (isign * swap_halves(v)).astype(bf16)], axis=0))
        e = dot(liy_ref[...], jnp.concatenate(both, axis=1)).astype(bf16)
        for i, xi in enumerate(pair):
            e_ref[xi * LANES : (xi + 1) * LANES, :] = e[:, i * LANES : (i + 1) * LANES]
    for xi in range(planes):
        here = pl.ds(xi * LANES, LANES)
        psi = dot(e_ref[here, :], wiz_ref[...]).astype(bf16)
        re, im = psi[:, :LANES], psi[:, LANES:]
        if keep_psi:
            psi_ref[0, xi] = re
            psi_ref[1, xi] = im
        re, im = re.astype(f32), im.astype(f32)
        total = (occ_ref[band] * scale) * (re * re + im * im)
        if adds:
            total = total + part_ref[here, :]
        if ends:
            write_rows(rho_refs, pl.program_id(0), planes * LANES, xi * LANES, total.astype(bf16), me)
        else:
            total_ref[here, :] = total


def inverse(me, blocks, occ, band, bands, liy, wiz, band_devices, scale, keep_psi, part):
    groups = len(blocks)
    per, slab, _ = blocks[0].shape
    planes = min(PLANES, slab)
    rows, block = slab * LANES, planes * LANES
    half = rows // band_devices // 2
    adds, ends = part is not None, band == bands - 1
    spec = pl.BlockSpec((per, planes, LANES), lambda s, m: (0, s, 0))
    rowspec = pl.BlockSpec((block, LANES), lambda s, m: (s, 0))
    const = lambda shape: pl.BlockSpec(shape, lambda s, m: (0,) * len(shape))
    outs, out_specs = [], []
    if keep_psi:
        outs.append(jax.ShapeDtypeStruct((2, 1, slab, LANES, LANES), bf16))
        out_specs.append(pl.BlockSpec((2, None, planes, LANES, LANES), lambda s, m: (0, 0, s, 0, 0)))
    if ends:
        outs += [jax.ShapeDtypeStruct((band_devices, half, LANES), bf16)] * 2
        out_specs += [const(outs[-1].shape)] * 2
    else:
        outs.append(jax.ShapeDtypeStruct((rows, LANES), f32))
        out_specs.append(rowspec)
    return pl.pallas_call(
        functools.partial(inverse_kernel, groups, planes, scale, band, adds, ends, keep_psi),
        grid_spec=pltpu.PrefetchScalarGridSpec(
            num_scalar_prefetch=1,
            grid=(slab // planes,),
            in_specs=[spec] * groups
            + [pl.BlockSpec(memory_space=pltpu.SMEM), table_spec(liy), const(wiz.shape)]
            + ([rowspec] if adds else []),
            out_specs=out_specs,
            scratch_shapes=[
                pltpu.VMEM((per * groups * planes, LANES), f32),
                pltpu.VMEM((block, LANES), bf16),
            ],
        ),
        out_shape=outs,
        compiler_params=pltpu.CompilerParams(vmem_limit_bytes=16 << 20),
        cost_estimate=pl.CostEstimate(flops=10**9, bytes_accessed=4 << 20, transcendentals=0),
        name="inverse",
    )(me, *blocks, occ, liy, wiz, *([part] if adds else []))


def partner(v, axis, size, mask):
    return lax.ppermute(v, axis, [(i, i ^ mask) for i in range(size)])


def exchange(blocks, axis, size):
    if size > 4:
        index = lax.axis_index(axis)
        order = jnp.arange(size, dtype=jnp.int32) ^ index
        stacked = jnp.stack(blocks)[order]
        got = lax.all_to_all(stacked, axis, 0, 0)[order]
        return [got[m] for m in range(size)]
    return [blocks[0]] + [partner(blocks[m], axis, size, m) for m in range(1, size)]


def add_pair(mine, got):
    return (mine.astype(f32) + got.astype(f32)).astype(bf16)


def reduce_blocks(upper, lower, axis, size, fill):
    both = [upper, lower]
    steps = list(zip(*orders(size)))
    for bits in steps[:-1]:
        cut = both[0].shape[0] // 2
        got = [partner(v[cut:], axis, size, 1 << bit) for v, bit in zip(both, bits)]
        if fill is not None:
            got, fill = lax.optimization_barrier((got, fill))
            filled, fill = fill, None
        both = [add_pair(v[:cut], g) for v, g in zip(both, got)]
    mine = jnp.concatenate(both, axis=0)
    return mine, partner(mine, axis, size, 1 << steps[-1][0]), filled


def gather_blocks(both, stats, axis, size, grid, grid_size):
    steps = list(reversed(list(zip(*orders(size)))[:-1]))
    stats = sum_direct(stats, grid, range(grid_size), grid_size)
    for i, bits in enumerate(steps):
        if i:
            both = [jnp.concatenate(v, axis=0) for v in both]
            both, stats = lax.optimization_barrier((both, stats))
        both = [[v, partner(v, axis, size, 1 << bit)] for v, bit in zip(both, bits)]
    return both[0] + both[1], sum_direct(stats, axis, range(size // 2), size)


def sum_direct(v, axis, masks, size):
    if size > 8:
        for bit in range(len(masks).bit_length() - 1):
            v = v + partner(v, axis, size, 1 << bit)
        return v
    terms = [v] + [partner(v, axis, size, m) for m in masks if m]
    while len(terms) > 1:
        terms = [terms[i] + terms[i + 1] for i in range(0, len(terms), 2)]
    return terms[0]


def local(
    bands,
    occupations,
    external,
    density_in,
    prev_density,
    prev_residual,
    hist_density,
    hist_residual,
):
    groups = lax.axis_size("grid")
    band_devices = lax.axis_size("band")
    slab, ng = external.shape[:2]
    nbands = bands.shape[1]
    cells = float(ng) ** 3
    scale = density_scale / (occupations.shape[0] * band_devices)
    rows = slab * ng
    kept = ng // 2
    per = kept // groups
    wz, wiz, ly, liy, lf, li = fourier_tables(ng, groups)
    grid_at = lax.axis_index("grid").astype(jnp.int32)
    shape = (per, kept, 2 * kept)
    squared = lambda v: ((v - kept // 2) * (v - kept // 2)).astype(f32)
    place = lambda d: lax.broadcasted_iota(jnp.int32, shape, d)
    radius = squared(place(0) + grid_at * per) + squared(place(1)) + squared(place(2) % kept)
    quarter = ng / 4.0
    kinetic = jnp.exp(-time_step * radius / (quarter * quarter))
    band_at = lax.axis_index("band").astype(jnp.int32)
    me = jnp.stack([band_at, grid_at])

    flat = lambda v: v.reshape(v.shape[:-3] + (rows, ng))
    ext, rho_in, prev_in, prev_res = map(flat, (external, density_in, prev_density, prev_residual))
    hist_r, hist_q = flat(hist_density), flat(hist_residual)
    psi = [(bands, b) for b in range(nbands)]
    block = rows // band_devices
    ends = jnp.stack([band_at, band_at ^ (band_devices // 2)])
    two = lambda v, axis, at: jnp.stack(
        [lax.dynamic_slice_in_dim(v, at[i] * block, block, axis) for i in range(2)], axis=axis
    )
    hist_pair, prev_res_pair = two(hist_q, 1, ends), two(prev_res, 0, ends)
    parts = max(1, slab // 8)
    extra = []
    new_q = []
    carry = None
    mix = None
    common = dict(ext=ext, wz=wz, ly=ly)
    for iteration in range(ITERS):
        blocks = []
        for b, (array, at) in enumerate(psi):
            if iteration and b == 0:
                out = forward("mix", me, slab, groups, cells, psi=array, band=at, mix=mix, **common)
                rho_in, carry = out[groups:]
            else:
                out = forward("plain", me, slab, groups, cells, psi=array, band=at, density=rho_in, **common)
            blocks.append(exchange(out[:groups], "grid", groups))
        for b in range(nbands):
            blocks[b] = exchange(x_filter(me, blocks[b], lf, li, kinetic), "grid", groups)
        last = iteration == ITERS - 1
        part = None
        psi = []
        for b in range(nbands):
            out = inverse(
                me, blocks[b], occupations, b, nbands, liy, wiz, band_devices, scale, not last, part
            )
            if not last:
                psi.append((out[0], 0))
                out = out[1:]
            part = out[0]
        out = list(out)
        if iteration == 0:
            out[0], tie, late_in = lax.optimization_barrier((out[0], ends, prev_in))
            fill = (
                [combine(tie, hist_r, hist_q, j, parts) for j in range(DEPTH - 1)],
                late_in + mixing_weight * prev_res,
            )
        else:
            out[0], rho, prev_mid = lax.optimization_barrier((out[0], mix["rho"], mix["prev_mid"]))
            prev_mid, newest_s = middle(me, slab, rho, mix["rho_in"], prev_mid)
            fill = (orig[1:], prev_mid, extra + [newest_s])
        mine, got, fill = reduce_blocks(out[0], out[1], "band", band_devices, fill)
        orig, prev_mid = fill[:2]
        if iteration:
            extra = fill[2]
        upper, lower = finish(mine, got)
        stats, newest_q, prev_res_pair = dots(
            iteration == 0, ends, upper, lower, rho_in, prev_res_pair, hist_pair, new_q
        )
        new_q = new_q + [newest_q]
        rho, stats = gather_blocks([upper, lower], stats, "band", band_devices, "grid", groups)
        mix = dict(stats=stats, carry=carry, rho=rho, rho_in=rho_in,
                   prev_mid=prev_mid, orig=orig, extra=extra)
    density, residual = forward("last", me, slab, groups, cells, mix=mix)
    unflat = lambda v: v.reshape(slab, ng, ng)
    return unflat(density), unflat(residual)


def solution(mesh):
    placed = (
        P(None, "band", "grid", None, None),
        P("band"),
        P("grid", None, None),
        P("grid", None, None),
        P("grid", None, None),
        P("grid", None, None),
        P(None, "grid", None, None),
        P(None, "grid", None, None),
    )
    return jax.shard_map(
        local,
        mesh=mesh,
        in_specs=placed,
        out_specs=(P("grid", None, None), P("grid", None, None)),
        check_vma=False,
    )
```

```python
import functools
import math

import jax
import jax.numpy as jnp
import ml_dtypes
import numpy as np
from jax import lax
from jax.experimental import pallas as pl
from jax.experimental.pallas import tpu as pltpu
from jax.sharding import PartitionSpec as P


DEPTH = 6
ITERS = 3
LANES = 128
PLANES = 16
FILTER_STEPS = 1

time_step = 0.25
energy_shift = 2.5
mixing_weight = 0.5
ridge_share = 0.1
ridge_floor = 0.01
density_scale = 8.0


f32 = jnp.float32
bf16 = jnp.bfloat16


def fourier_tables(length, groups):
    frequency = np.arange(-(length // 4), length // 4)
    phase_index = np.arange(length)[:, None] * frequency[None, :] % length
    angles = phase_index.astype(np.float32) * np.float32(2.0 * math.pi / length)
    unit_scale = np.float32(1.0 / math.sqrt(length))
    cos, sin = (f(angles).astype(np.float32) * unit_scale for f in (np.cos, np.sin))
    out = [
        np.block([[cos, -sin], [sin, cos]]),
        np.block([[cos.T, sin.T], [-sin.T, cos.T]]),
    ]
    stacks = [[], [], [], []]
    for index in range(groups):
        def ordered(count):
            return np.concatenate([np.arange(count // groups) + (index ^ m) * (count // groups) for m in range(groups)])

        ck, sk = (v[:, ordered(len(frequency))] for v in (cos, sin))
        cx, sx = (v[ordered(length)] for v in (cos, sin))
        stacks[0].append(np.concatenate([ck.T, sk.T], axis=0))
        stacks[1].append(np.concatenate([ck, sk], axis=1))
        stacks[2].append(np.concatenate([cx.T, sx.T], axis=0))
        stacks[3].append(np.concatenate([cx, sx], axis=1))
    return [jnp.asarray(v.astype(ml_dtypes.bfloat16)) for v in out + [np.stack(v) for v in stacks]]


def dot(a, b):
    return jnp.dot(a, b, preferred_element_type=f32)


def swap_halves(v):
    return pltpu.roll(v, v.shape[-1] // 2, v.ndim - 1)


def half_sign(shape, first):
    lane = lax.broadcasted_iota(jnp.int32, shape, len(shape) - 1)
    return jnp.where(lane < shape[-1] // 2, first, -first).astype(f32)


def orders(devices):
    bits = devices.bit_length() - 1
    upper = list(range(bits))
    lower = ([1, 0] + upper[2:]) if bits > 1 else upper
    return upper, lower


def position(relative, order):
    out = None
    for i, bit in enumerate(order):
        part = lax.shift_left(lax.bitwise_and(lax.shift_right_logical(relative, bit), 1), len(order) - 1 - i)
        out = part if out is None else out + part
    return out


def units(half, devices, step, step_rows, row, count, me):
    assert step_rows % (2 * half) == 0
    unit = min(count, half)
    for at in range(0, count, unit):
        block, within = divmod(row + at, 2 * half)
        which, offset = divmod(within, half)
        relative = lax.bitwise_xor(step * (step_rows // (2 * half)) + block, me)
        yield which, position(relative, orders(devices)[which]), offset, at, unit


def read_rows(refs, step, step_rows, row, count, me):
    near, half = refs[0].shape[:2]
    out = []
    for which, at, offset, _, unit in units(half, 2 * near, step, step_rows, row, count, me):
        here = (lax.rem(at, near), pl.ds(offset, unit), slice(None))
        low, high = (refs[2 * which + i][here].astype(f32) for i in range(2))
        out.append(jnp.where(at < near, low, high))
    return out[0] if len(out) == 1 else jnp.concatenate(out, axis=0)


def write_rows(refs, step, step_rows, row, value, me):
    devices, half = refs[0].shape[:2]
    for which, to, offset, at, unit in units(half, devices, step, step_rows, row, value.shape[0], me):
        refs[which][to, pl.ds(offset, unit), :] = value[at : at + unit]


def solve_rows(gram, rhs):
    n = len(rhs)
    trace = gram[0][0]
    for j in range(1, n):
        trace = trace + gram[j][j]
    ridge = ridge_share * trace / n + ridge_floor
    a = [[gram[j][k] + ridge if j == k else gram[j][k] for k in range(n)] for j in range(n)]
    low = [[None] * n for _ in range(n)]
    diag = [None] * n
    inv = [None] * n
    for j in range(n):
        value = a[j][j]
        scaled = []
        for k in range(j):
            s = low[j][k] * diag[k]
            scaled.append(s)
            value = value - low[j][k] * s
        diag[j] = value
        inv[j] = 1.0 / value
        for r in range(j + 1, n):
            e = a[r][j]
            for k in range(j):
                e = e - low[r][k] * scaled[k]
            low[r][j] = e * inv[j]
    mid = []
    for j in range(n):
        e = rhs[j]
        for k in range(j):
            e = e - low[j][k] * mid[k]
        mid.append(e)
    out = [None] * n
    for j in reversed(range(n)):
        e = mid[j] * inv[j]
        for k in range(j + 1, n):
            e = e - low[k][j] * out[k]
        out[j] = e
    return out


def pair_index(n):
    return {(j, k): i for i, (j, k) in enumerate((j, k) for j in range(n) for k in range(j, n))}


STAT_ROWS = 32


def spread_diagonal(row):
    shape = (STAT_ROWS, LANES)
    lane = lax.broadcasted_iota(jnp.int32, shape, 1)
    own = lax.broadcasted_iota(jnp.int32, shape, 0)
    picked = jnp.where(lane == own, jnp.broadcast_to(row, shape), 0.0)
    return jnp.broadcast_to(jnp.sum(picked, axis=1, keepdims=True), shape)


def finish_stats(stats_ref, carry_ref, first, cells):
    total = spread_diagonal(stats_ref[...] * (1.0 / cells))
    n = DEPTH
    gram = [[None] * n for _ in range(n)]
    kept = pair_index(n - 1)
    for (j, k), i in kept.items():
        value = total[2 * n + i : 2 * n + i + 1] if first else carry_ref[i : i + 1, :]
        gram[j][k] = value
        gram[k][j] = value
    for j in range(n):
        value = total[j : j + 1]
        gram[j][n - 1] = value
        gram[n - 1][j] = value
    rhs = [total[n + j : n + j + 1] for j in range(n)]
    return gram, rhs


CARRY_ROWS = 16


def combine_kernel(tie_ref, r_ref, q_ref, s_ref):
    s_ref[...] = (r_ref[...] + mixing_weight * q_ref[...]).astype(s_ref.dtype)


def combine(tie, hist_density, hist_residual, j, parts):
    _, rows, lanes = hist_density.shape
    block = rows // parts
    spec = pl.BlockSpec((None, block, lanes), lambda s, t: (j, s, 0))
    return pl.pallas_call(
        combine_kernel,
        grid_spec=pltpu.PrefetchScalarGridSpec(
            num_scalar_prefetch=1,
            grid=(parts,),
            in_specs=[spec, spec],
            out_specs=pl.BlockSpec((block, lanes), lambda s, t: (s, 0)),
        ),
        out_shape=jax.ShapeDtypeStruct((rows, lanes), bf16),
        compiler_params=pltpu.CompilerParams(vmem_limit_bytes=12 << 20),
        cost_estimate=pl.CostEstimate(flops=10**8, bytes_accessed=rows * lanes * 10, transcendentals=0),
        name="combine",
    )(tie, hist_density, hist_residual)


def middle_kernel(me_ref, *refs):
    rho_refs, (in_ref, prev_ref, mid_ref, new_ref) = refs[:4], refs[4:]
    rows = in_ref.shape[0]
    for base in range(0, rows, LANES):
        here = pl.ds(base, LANES)
        rho_out = read_rows(rho_refs, pl.program_id(0), rows, base, LANES, me_ref[0])
        mid = mixing_weight * (rho_out + in_ref[here, :])
        mid_ref[here, :] = mid
        new_ref[here, :] = (mid - prev_ref[here, :]).astype(new_ref.dtype)


def middle(me, slab, rho, rho_in, prev_mid):
    planes = min(PLANES, slab)
    rows, block = rho_in.shape[0], planes * LANES
    spec = pl.BlockSpec((block, LANES), lambda s, m: (s, 0))
    const = lambda shape: pl.BlockSpec(shape, lambda s, m: (0,) * len(shape))
    return pl.pallas_call(
        middle_kernel,
        grid_spec=pltpu.PrefetchScalarGridSpec(
            num_scalar_prefetch=1,
            grid=(rows // block,),
            in_specs=[const(v.shape) for v in rho] + [spec, spec],
            out_specs=[spec, spec],
        ),
        out_shape=[jax.ShapeDtypeStruct((rows, LANES), f32), jax.ShapeDtypeStruct((rows, LANES), bf16)],
        compiler_params=pltpu.CompilerParams(vmem_limit_bytes=12 << 20),
        cost_estimate=pl.CostEstimate(flops=10**8, bytes_accessed=rows * LANES * 12, transcendentals=0),
        name="middle",
    )(me, *rho, rho_in, prev_mid)


def row_sum(v):
    return jnp.sum(v, axis=0, keepdims=True)


def finish_kernel(mine_ref, got_ref, sum_ref):
    for i in range(2):
        sum_ref[i] = (mine_ref[i].astype(f32) + got_ref[1 - i].astype(f32)).astype(bf16)


def finish(mine, got):
    return pl.pallas_call(
        finish_kernel,
        out_shape=jax.ShapeDtypeStruct(mine.shape, bf16),
        compiler_params=pltpu.CompilerParams(vmem_limit_bytes=8 << 20),
        cost_estimate=pl.CostEstimate(flops=10**6, bytes_accessed=3 * mine.size, transcendentals=0),
        name="finish",
    )(mine, got)


def dots_kernel(first, at_ref, *refs):
    q_count = DEPTH - 1
    upper_ref, lower_ref, own_in, far_in, prev_ref, hist_ref = refs[:6]
    recent, (stats_ref, newest_ref, res_ref) = refs[6:-3], refs[-3:]
    half = upper_ref.shape[1]
    total = None
    for side, in_ref in enumerate((own_in, far_in)):
        rows = []
        for part in range(2):
            here = slice(part * half, (part + 1) * half)
            q = [hist_ref[j, side, here, :] for j in range(len(recent), q_count)] + [r[side, here, :] for r in recent]
            res = (upper_ref, lower_ref)[part][side].astype(f32) - in_ref[here, :]
            newest = res - prev_ref[side, here, :]
            newest_ref[side, here, :] = newest
            res_ref[side, here, :] = res
            out = [row_sum(v * newest) for v in q] + [row_sum(newest * newest)]
            out += [row_sum(v * res) for v in q] + [row_sum(newest * res)]
            if first:
                for j, k in pair_index(q_count):
                    out.append(row_sum(q[j] * q[k]))
            out += [jnp.zeros((1, LANES), f32)] * (STAT_ROWS - len(out))
            rows.append(jnp.concatenate(out, axis=0))
        table = rows[0] + rows[1]
        total = table if total is None else total + table
    table = jnp.sum(total, axis=1, keepdims=True)
    shape = (STAT_ROWS, LANES)
    lane = lax.broadcasted_iota(jnp.int32, shape, 1)
    own = lax.broadcasted_iota(jnp.int32, shape, 0)
    stats_ref[...] = row_sum(jnp.where(lane == own, jnp.broadcast_to(table, shape), 0.0))


def dots(first, at, upper, lower, rho_in, prev_res, hist, recent):
    half = upper.shape[1]
    block = 2 * half
    const = lambda shape: pl.BlockSpec(shape, lambda s, m: (0,) * len(shape))
    pair = (2, block, LANES)
    return pl.pallas_call(
        functools.partial(dots_kernel, first),
        grid_spec=pltpu.PrefetchScalarGridSpec(
            num_scalar_prefetch=1,
            grid=(1,),
            in_specs=[
                const(upper.shape),
                const(lower.shape),
                pl.BlockSpec((block, LANES), lambda s, m: (m[0], 0)),
                pl.BlockSpec((block, LANES), lambda s, m: (m[1], 0)),
                const(pair),
                const(hist.shape),
            ]
            + [const(pair)] * len(recent),
            out_specs=[const((1, LANES)), const(pair), const(pair)],
        ),
        out_shape=[
            jax.ShapeDtypeStruct((1, LANES), f32),
            jax.ShapeDtypeStruct(pair, f32),
            jax.ShapeDtypeStruct(pair, f32),
        ],
        compiler_params=pltpu.CompilerParams(vmem_limit_bytes=14 << 20),
        cost_estimate=pl.CostEstimate(flops=1, bytes_accessed=block * LANES * 64, transcendentals=0),
        name="dots",
    )(at, upper, lower, rho_in, rho_in, prev_res, hist, *recent)


def mix_plane(me, coeffs, step, step_rows, base, rows, rho_refs, in_ref, prev_mid_ref, s_refs):
    rho_out = read_rows(rho_refs, step, step_rows, base, rows, me)
    here = pl.ds(base, rows)
    rho_in = in_ref[here, :]
    mid = mixing_weight * (rho_out + rho_in)
    dens = mid - coeffs[-1] * (mid - prev_mid_ref[here, :])
    for c, ref in zip(coeffs, s_refs):
        dens = dens - c * ref[here, :].astype(f32)
    return dens, rho_out - rho_in


def forward_kernel(kind, planes, first, groups, cells, me_ref, *refs):
    refs = list(refs)
    take = lambda k: [refs.pop(0) for _ in range(k)]
    mixing = kind != "plain"
    me = me_ref[0]
    if mixing:
        (stats_ref,) = take(1)
        carry_ref = None if first else take(1)[0]
        rho_refs = take(4)
        in_ref, prev_mid_ref = take(2)
        s_refs = take(DEPTH - 1)
    else:
        (in_ref,) = take(1)
    if kind != "last":
        ext_ref, psi_ref, wz_ref, ly_ref = take(4)
        out_refs = take(groups)
    if mixing:
        dens_ref, second = take(2)
        (coeff_ref,) = take(1)

        @pl.when(pl.program_id(0) == 0)
        def _():
            gram, rhs = finish_stats(stats_ref, carry_ref, first, cells)
            for j, c in enumerate(solve_rows(gram, rhs)):
                coeff_ref[j : j + 1, :] = c
            if kind == "mix":
                second[...] = jnp.zeros_like(second)
                for (j, k), i in pair_index(DEPTH - 1).items():
                    second[i : i + 1, :] = gram[j + 1][k + 1]

        coeffs = [coeff_ref[j : j + 1, :] for j in range(DEPTH)]
    if kind != "last":
        w_ref, a_ref, scratch = take(3)
    for xi in range(planes):
        here = pl.ds(xi * LANES, LANES)
        if mixing:
            dens, res = mix_plane(
                me, coeffs, pl.program_id(0), planes * LANES, xi * LANES, LANES,
                rho_refs, in_ref, prev_mid_ref, s_refs,
            )
            dens_ref[here, :] = dens
            if kind == "last":
                second[here, :] = res
        else:
            dens = in_ref[here, :]
        if kind != "last":
            factor = jnp.exp(-time_step * (ext_ref[here, :] + dens - energy_shift))
            for c in range(2):
                w_ref[here, c * LANES : (c + 1) * LANES] = (psi_ref[c, xi].astype(f32) * factor).astype(bf16)
    if kind == "last":
        return
    kept = ly_ref.shape[0] // 2
    sign = half_sign((kept, LANES), 1.0)
    a_ref[...] = dot(w_ref[...], wz_ref[...]).astype(bf16)
    for pair in pairs(planes):
        wide = [a_ref[xi * LANES : (xi + 1) * LANES, :] for xi in pair]
        t = dot(ly_ref[...], jnp.concatenate(wide, axis=1))
        for i, xi in enumerate(pair):
            lanes = slice(i * LANES, (i + 1) * LANES)
            out = t[:kept, lanes] + sign * swap_halves(t[kept:, lanes])
            scratch[pl.ds(xi, kept, stride=planes), :] = out
    per = kept // groups
    for g in range(groups):
        rows = scratch[g * per * planes : (g + 1) * per * planes, :]
        out_refs[g][...] = rows.reshape(per, planes, LANES).astype(bf16)


def table_spec(table):
    return pl.BlockSpec((None,) + table.shape[1:], lambda s, m: (m[1], 0, 0))


def pairs(count):
    return [tuple(range(i, min(i + 2, count))) for i in range(0, count, 2)]


def forward(kind, me, slab, groups, cells, ext=None, psi=None, band=0, wz=None, ly=None, density=None, mix=None):
    planes = min(PLANES, slab)
    steps = slab // planes
    block = planes * LANES
    rows = slab * LANES
    const = lambda shape: pl.BlockSpec(shape, lambda s, m: (0,) * len(shape))
    rowspec = pl.BlockSpec((block, LANES), lambda s, m: (s, 0))
    args, specs, outs, out_specs, scratch = [], [], [], [], []
    first = False
    if kind != "plain":
        first = mix["carry"] is None
        small = [mix["stats"]] + ([] if first else [mix["carry"]]) + list(mix["rho"])
        args += small
        specs += [const(v.shape) for v in small]
        wide = [mix["rho_in"], mix["prev_mid"]] + list(mix["orig"]) + list(mix["extra"])
        args += wide
        specs += [rowspec] * len(wide)
    else:
        args.append(density)
        specs.append(rowspec)
    if kind != "last":
        kept = ly.shape[1] // 2
        per = kept // groups
        args += [ext, psi, wz, ly]
        specs += [
            rowspec,
            pl.BlockSpec((2, None, planes, LANES, LANES), lambda s, m: (0, band, s, 0, 0)),
            const(wz.shape),
            table_spec(ly),
        ]
        outs += [jax.ShapeDtypeStruct((per, slab, LANES), bf16)] * groups
        out_specs += [pl.BlockSpec((per, planes, LANES), lambda s, m: (0, s, 0))] * groups
    if kind != "plain":
        outs.append(jax.ShapeDtypeStruct((rows, LANES), f32))
        out_specs.append(rowspec)
        if kind == "mix":
            outs.append(jax.ShapeDtypeStruct((CARRY_ROWS, LANES), f32))
            out_specs.append(const((CARRY_ROWS, LANES)))
        else:
            outs.append(jax.ShapeDtypeStruct((rows, LANES), f32))
            out_specs.append(rowspec)
        scratch.append(pltpu.VMEM((8, LANES), f32))
    if kind != "last":
        scratch += [
            pltpu.VMEM((block, 2 * LANES), bf16),
            pltpu.VMEM((block, LANES), bf16),
            pltpu.VMEM((kept * planes, LANES), f32),
        ]
    return pl.pallas_call(
        functools.partial(forward_kernel, kind, planes, first, groups, cells),
        grid_spec=pltpu.PrefetchScalarGridSpec(
            num_scalar_prefetch=1, grid=(steps,), in_specs=specs, out_specs=out_specs, scratch_shapes=scratch
        ),
        out_shape=outs,
        compiler_params=pltpu.CompilerParams(vmem_limit_bytes=20 << 20),
        cost_estimate=pl.CostEstimate(flops=10**9, bytes_accessed=6 << 20, transcendentals=0),
    )(me, *args)


def filter_kernel(groups, me_ref, *refs):
    in_refs, refs = refs[:groups], refs[groups:]
    lf_ref, li_ref, kin_ref = refs[:3]
    out_refs = refs[3:]
    per, slab, _ = in_refs[0].shape
    kept = lf_ref.shape[0] // 2
    fsign = half_sign((kept, LANES), 1.0)
    isign = half_sign((kept, LANES), -1.0)
    for pair in pairs(per):
        wide = [jnp.concatenate([r[k] for r in in_refs], axis=0) for k in pair]
        t = dot(lf_ref[...], jnp.concatenate(wide, axis=1))
        both = []
        for i, k in enumerate(pair):
            lanes = slice(i * LANES, (i + 1) * LANES)
            c = (t[:kept, lanes] + fsign * swap_halves(t[kept:, lanes])) * kin_ref[k]
            both.append(jnp.concatenate([c.astype(bf16), (isign * swap_halves(c)).astype(bf16)], axis=0))
        d = dot(li_ref[...], jnp.concatenate(both, axis=1)).astype(bf16)
        for i, k in enumerate(pair):
            for g in range(groups):
                out_refs[g][k] = d[g * slab : (g + 1) * slab, i * LANES : (i + 1) * LANES]


def x_filter(me, blocks, lf, li, kinetic):
    groups = len(blocks)
    per, slab, _ = blocks[0].shape
    split = FILTER_STEPS if per % (2 * FILTER_STEPS) == 0 else 1
    spec = pl.BlockSpec((per // split, slab, LANES), lambda s, m: (s, 0, 0))
    return pl.pallas_call(
        functools.partial(filter_kernel, groups),
        grid_spec=pltpu.PrefetchScalarGridSpec(
            num_scalar_prefetch=1,
            grid=(split,),
            in_specs=[spec] * groups
            + [
                table_spec(lf),
                table_spec(li),
                pl.BlockSpec((per // split,) + kinetic.shape[1:], lambda s, m: (s, 0, 0)),
            ],
            out_specs=[spec] * groups,
        ),
        out_shape=[jax.ShapeDtypeStruct(blocks[0].shape, bf16)] * groups,
        compiler_params=pltpu.CompilerParams(vmem_limit_bytes=12 << 20),
        cost_estimate=pl.CostEstimate(flops=5 * 10**8, bytes_accessed=2 << 20, transcendentals=0),
        name="x_filter",
    )(me, *blocks, lf, li, kinetic)


def inverse_kernel(groups, planes, scale, band, adds, ends, keep_psi, me_ref, *refs):
    in_refs, refs = refs[:groups], refs[groups:]
    occ_ref, liy_ref, wiz_ref = refs[:3]
    refs = list(refs[3:])
    if adds:
        part_ref = refs.pop(0)
    if keep_psi:
        psi_ref = refs.pop(0)
    if ends:
        rho_refs = [refs.pop(0) for _ in range(2)]
    else:
        total_ref = refs.pop(0)
    scratch, e_ref = refs
    me = me_ref[0]
    per = in_refs[0].shape[0]
    kept = per * groups
    isign = half_sign((kept, LANES), -1.0)
    for g in range(groups):
        scratch[g * per * planes : (g + 1) * per * planes, :] = (
            in_refs[g][...].astype(f32).reshape(per * planes, LANES)
        )
    for pair in pairs(planes):
        both = []
        for xi in pair:
            v = scratch[pl.ds(xi, kept, stride=planes), :]
            both.append(jnp.concatenate([v.astype(bf16), (isign * swap_halves(v)).astype(bf16)], axis=0))
        e = dot(liy_ref[...], jnp.concatenate(both, axis=1)).astype(bf16)
        for i, xi in enumerate(pair):
            e_ref[xi * LANES : (xi + 1) * LANES, :] = e[:, i * LANES : (i + 1) * LANES]
    for xi in range(planes):
        here = pl.ds(xi * LANES, LANES)
        psi = dot(e_ref[here, :], wiz_ref[...]).astype(bf16)
        re, im = psi[:, :LANES], psi[:, LANES:]
        if keep_psi:
            psi_ref[0, xi] = re
            psi_ref[1, xi] = im
        re, im = re.astype(f32), im.astype(f32)
        total = (occ_ref[band] * scale) * (re * re + im * im)
        if adds:
            total = total + part_ref[here, :]
        if ends:
            write_rows(rho_refs, pl.program_id(0), planes * LANES, xi * LANES, total.astype(bf16), me)
        else:
            total_ref[here, :] = total


def inverse(me, blocks, occ, band, bands, liy, wiz, band_devices, scale, keep_psi, part):
    groups = len(blocks)
    per, slab, _ = blocks[0].shape
    planes = min(PLANES, slab)
    rows, block = slab * LANES, planes * LANES
    half = rows // band_devices // 2
    adds, ends = part is not None, band == bands - 1
    spec = pl.BlockSpec((per, planes, LANES), lambda s, m: (0, s, 0))
    rowspec = pl.BlockSpec((block, LANES), lambda s, m: (s, 0))
    const = lambda shape: pl.BlockSpec(shape, lambda s, m: (0,) * len(shape))
    outs, out_specs = [], []
    if keep_psi:
        outs.append(jax.ShapeDtypeStruct((2, 1, slab, LANES, LANES), bf16))
        out_specs.append(pl.BlockSpec((2, None, planes, LANES, LANES), lambda s, m: (0, 0, s, 0, 0)))
    if ends:
        outs += [jax.ShapeDtypeStruct((band_devices, half, LANES), bf16)] * 2
        out_specs += [const(outs[-1].shape)] * 2
    else:
        outs.append(jax.ShapeDtypeStruct((rows, LANES), f32))
        out_specs.append(rowspec)
    return pl.pallas_call(
        functools.partial(inverse_kernel, groups, planes, scale, band, adds, ends, keep_psi),
        grid_spec=pltpu.PrefetchScalarGridSpec(
            num_scalar_prefetch=1,
            grid=(slab // planes,),
            in_specs=[spec] * groups
            + [pl.BlockSpec(memory_space=pltpu.SMEM), table_spec(liy), const(wiz.shape)]
            + ([rowspec] if adds else []),
            out_specs=out_specs,
            scratch_shapes=[
                pltpu.VMEM((per * groups * planes, LANES), f32),
                pltpu.VMEM((block, LANES), bf16),
            ],
        ),
        out_shape=outs,
        compiler_params=pltpu.CompilerParams(vmem_limit_bytes=16 << 20),
        cost_estimate=pl.CostEstimate(flops=10**9, bytes_accessed=4 << 20, transcendentals=0),
        name="inverse",
    )(me, *blocks, occ, liy, wiz, *([part] if adds else []))


def partner(v, axis, size, mask):
    return lax.ppermute(v, axis, [(i, i ^ mask) for i in range(size)])


def exchange(blocks, axis, size):
    if size > 4:
        index = lax.axis_index(axis)
        order = jnp.arange(size, dtype=jnp.int32) ^ index
        stacked = jnp.stack(blocks)[order]
        got = lax.all_to_all(stacked, axis, 0, 0)[order]
        return [got[m] for m in range(size)]
    return [blocks[0]] + [partner(blocks[m], axis, size, m) for m in range(1, size)]


def add_pair(mine, got):
    return (mine.astype(f32) + got.astype(f32)).astype(bf16)


def reduce_blocks(upper, lower, axis, size, fill):
    both = [upper, lower]
    steps = list(zip(*orders(size)))
    for bits in steps[:-1]:
        cut = both[0].shape[0] // 2
        got = [partner(v[cut:], axis, size, 1 << bit) for v, bit in zip(both, bits)]
        if fill is not None:
            got, fill = lax.optimization_barrier((got, fill))
            filled, fill = fill, None
        both = [add_pair(v[:cut], g) for v, g in zip(both, got)]
    return both, [partner(v, axis, size, 1 << bit) for v, bit in zip(both, steps[-1])], filled


def gather_blocks(both, stats, axis, size, grid, grid_size):
    steps = list(reversed(list(zip(*orders(size)))[:-1]))
    stats = sum_direct(stats, grid, range(grid_size), grid_size)
    for i, bits in enumerate(steps):
        if i:
            both = [jnp.concatenate(v, axis=0) for v in both]
            both, stats = lax.optimization_barrier((both, stats))
        both = [[v, partner(v, axis, size, 1 << bit)] for v, bit in zip(both, bits)]
    return both[0] + both[1], sum_direct(stats, axis, range(size // 2), size)


def sum_direct(v, axis, masks, size):
    if size > 8:
        for bit in range(len(masks).bit_length() - 1):
            v = v + partner(v, axis, size, 1 << bit)
        return v
    terms = [v] + [partner(v, axis, size, m) for m in masks if m]
    while len(terms) > 1:
        terms = [terms[i] + terms[i + 1] for i in range(0, len(terms), 2)]
    return terms[0]


def local(
    bands,
    occupations,
    external,
    density_in,
    prev_density,
    prev_residual,
    hist_density,
    hist_residual,
):
    groups = lax.axis_size("grid")
    band_devices = lax.axis_size("band")
    slab, ng = external.shape[:2]
    nbands = bands.shape[1]
    cells = float(ng) ** 3
    scale = density_scale / (occupations.shape[0] * band_devices)
    rows = slab * ng
    kept = ng // 2
    per = kept // groups
    wz, wiz, ly, liy, lf, li = fourier_tables(ng, groups)
    grid_at = lax.axis_index("grid").astype(jnp.int32)
    shape = (per, kept, 2 * kept)
    squared = lambda v: ((v - kept // 2) * (v - kept // 2)).astype(f32)
    place = lambda d: lax.broadcasted_iota(jnp.int32, shape, d)
    radius = squared(place(0) + grid_at * per) + squared(place(1)) + squared(place(2) % kept)
    quarter = ng / 4.0
    kinetic = jnp.exp(-time_step * radius / (quarter * quarter))
    band_at = lax.axis_index("band").astype(jnp.int32)
    me = jnp.stack([band_at, grid_at])

    flat = lambda v: v.reshape(v.shape[:-3] + (rows, ng))
    ext, rho_in, prev_in, prev_res = map(flat, (external, density_in, prev_density, prev_residual))
    hist_r, hist_q = flat(hist_density), flat(hist_residual)
    psi = [(bands, b) for b in range(nbands)]
    block = rows // band_devices
    ends = jnp.stack([band_at, band_at ^ (band_devices // 2)])
    two = lambda v, axis, at: jnp.stack(
        [lax.dynamic_slice_in_dim(v, at[i] * block, block, axis) for i in range(2)], axis=axis
    )
    hist_pair, prev_res_pair = two(hist_q, 1, ends), two(prev_res, 0, ends)
    parts = max(1, slab // 8)
    extra = []
    new_q = []
    carry = None
    mix = None
    common = dict(ext=ext, wz=wz, ly=ly)
    for iteration in range(ITERS):
        blocks = []
        for b, (array, at) in enumerate(psi):
            if iteration and b == 0:
                out = forward("mix", me, slab, groups, cells, psi=array, band=at, mix=mix, **common)
                rho_in, carry = out[groups:]
            else:
                out = forward("plain", me, slab, groups, cells, psi=array, band=at, density=rho_in, **common)
            blocks.append(exchange(out[:groups], "grid", groups))
        for b in range(nbands):
            blocks[b] = exchange(x_filter(me, blocks[b], lf, li, kinetic), "grid", groups)
        last = iteration == ITERS - 1
        part = None
        psi = []
        for b in range(nbands):
            out = inverse(
                me, blocks[b], occupations, b, nbands, liy, wiz, band_devices, scale, not last, part
            )
            if not last:
                psi.append((out[0], 0))
                out = out[1:]
            part = out[0]
        out = list(out)
        if iteration == 0:
            out[0], tie, late_in = lax.optimization_barrier((out[0], ends, prev_in))
            fill = (
                [combine(tie, hist_r, hist_q, j, parts) for j in range(DEPTH - 1)],
                late_in + mixing_weight * prev_res,
            )
        else:
            out[0], rho, prev_mid = lax.optimization_barrier((out[0], mix["rho"], mix["prev_mid"]))
            prev_mid, newest_s = middle(me, slab, rho, mix["rho_in"], prev_mid)
            fill = (orig[1:], prev_mid, extra + [newest_s])
        mine, got, fill = reduce_blocks(out[0], out[1], "band", band_devices, fill)
        orig, prev_mid = fill[:2]
        if iteration:
            extra = fill[2]
        upper, lower = (finish(m, g) for m, g in zip(mine, got))
        stats, newest_q, prev_res_pair = dots(
            iteration == 0, ends, upper, lower, rho_in, prev_res_pair, hist_pair, new_q
        )
        new_q = new_q + [newest_q]
        rho, stats = gather_blocks([upper, lower], stats, "band", band_devices, "grid", groups)
        mix = dict(stats=stats, carry=carry, rho=rho, rho_in=rho_in,
                   prev_mid=prev_mid, orig=orig, extra=extra)
    density, residual = forward("last", me, slab, groups, cells, mix=mix)
    unflat = lambda v: v.reshape(slab, ng, ng)
    return unflat(density), unflat(residual)


def solution(mesh):
    placed = (
        P(None, "band", "grid", None, None),
        P("band"),
        P("grid", None, None),
        P("grid", None, None),
        P("grid", None, None),
        P("grid", None, None),
        P(None, "grid", None, None),
        P(None, "grid", None, None),
    )
    return jax.shard_map(
        local,
        mesh=mesh,
        in_specs=placed,
        out_specs=(P("grid", None, None), P("grid", None, None)),
        check_vma=False,
    )
```
